512 devices in a mesh: tm: 32 (over y, z_lo), space: 16 (over x, z_hi, core).
Axes of the slice: x: 4, y: 8, z: 8 (z_hi: 2, z_lo: 4; z = z_hi * 4 + z_lo), core: 2. Of those that a mesh axis runs over, the one named last changes fastest.
Arguments:
- c_points: float32 [32, 256, 32, 128], P('tm', 'space'), may hold values from -15 to 15
- corrections: float32 [32, 256, 32, 128], P('tm', 'space'), may hold values from -3 to 3
- conductivity: float32 [256, 32, 128], P('space'), may hold values from 0.2 to 5
- forcing: float32 [256, 32, 128], P('space'), may hold values from -6 to 6
Outputs:
- f_states: float32 [32, 2, 256, 32, 128], P('tm', None, 'space')
The draws below stay inside these ranges and needn't reach their ends.
All inputs are finite; a program needn't handle non-finite values.
Results may differ from the reference program's by a relative error of at most 0.0002.
Values sent between devices are 32-bit elements; how exact they have to be, the bound alone decides.
A program may use at most 64 MiB of HBM per device.

```python
import math
import jax
import jax.numpy as jnp
from jax import lax

NY = 32
NX = 128
ITERS = 6
STEPS = 2
GROUPS = 32
NZ = 256


def draw_c_points(key, part):
    depth_frac = jnp.arange(NZ, dtype=jnp.float32) / max(NZ - 1, 1)
    depth_scale = (1.0 + 2.0 * depth_frac)[None, :, None, None]
    random_part = jax.random.normal(key, (GROUPS, NZ, NY, NX), jnp.float32)
    values = depth_scale * random_part
    return jnp.clip(values, -15.0, 15.0)


def block_levels(key, shape, cuts, smallest, largest):
    factor_of = 1.0
    for dim, parts in cuts:
        heights = jax.random.uniform(jax.random.fold_in(jax.random.fold_in(key, 6), dim), (parts,), jnp.float32, smallest / len(cuts), largest / len(cuts))
        factor_of = factor_of * jnp.repeat(jnp.exp(heights), shape[dim] // parts).reshape((-1,) + (1,) * (len(shape) - 1 - dim))
    return factor_of


def gaussian(key, extent, spread, most, shards=(), kind=jnp.bfloat16):
    factor_of = block_levels(key, extent, shards, -0.22, 0.18) if shards else 1.0
    entries = jax.random.normal(key, extent, jnp.float32) * spread * factor_of
    return jnp.minimum(jnp.maximum(entries, -most), most).astype(kind)


def setup_inputs(seed: int = 0) -> dict:
    keys = jax.random.split(jax.random.key(seed), 5)
    return {
        "c_points": draw_c_points(jax.random.fold_in(keys[4], 71), 0),
        "corrections": gaussian(keys[1], (GROUPS, NZ, NY, NX), 0.5, 3.0, ((0, 32), (1, 16)), jnp.float32),
        "conductivity": jnp.clip(jnp.exp(math.log(5.0) - 3.218876 * jax.random.uniform(keys[2], (NZ, NY, NX), jnp.float32) ** block_levels(keys[2], (NZ, NY, NX), ((0, 16),), -0.2, 0.2)), 0.2, 5.0),
        "forcing": gaussian(keys[3], (NZ, NY, NX), 1.0, 6.0, ((0, 16),), jnp.float32),
    }


step_rate = 4.0
source_weight = 0.25


def neighbours(padded):
    return (padded[2:, 1:-1, 1:-1], padded[:-2, 1:-1, 1:-1],
            padded[1:-1, 2:, 1:-1], padded[1:-1, :-2, 1:-1],
            padded[1:-1, 1:-1, 2:], padded[1:-1, 1:-1, :-2])


def faces_of(padded_conductivity):
    centre = padded_conductivity[1:-1, 1:-1, 1:-1]
    return tuple(0.5 * (centre + beside) for beside in neighbours(padded_conductivity))


def apply_operator(grid_field, padded, face_weights):
    flux_sum = jnp.zeros_like(grid_field)
    for face_weight, beside in zip(face_weights, neighbours(padded)):
        flux_sum = flux_sum + face_weight * (grid_field - beside)
    return grid_field + step_rate * flux_sum


def reference(c_points, corrections, conductivity, forcing):
    face_weights = faces_of(jnp.pad(conductivity, 1))

    def operate(grid_field):
        return apply_operator(grid_field, jnp.pad(grid_field, 1), face_weights)

    def advance(start_value):
        current = start_value
        sections = []
        for section in range(STEPS):
            right_side = current + source_weight * forcing
            solution = current
            residual = right_side - operate(current)
            direction = residual
            norm_now = jnp.sum(residual * residual)
            for sweep in range(ITERS):
                applied = operate(direction)
                step_length = norm_now / jnp.sum(direction * applied)
                solution = solution + step_length * direction
                if sweep + 1 < ITERS:
                    residual = residual - step_length * applied
                    norm_next = jnp.sum(residual * residual)
                    direction = residual + (norm_next / norm_now) * direction
                    norm_now = norm_next
            sections.append(solution)
            current = solution
        return jnp.stack(sections)

    prior_fix = jnp.concatenate([jnp.zeros_like(corrections[:1]), corrections[:-1]], axis=0)
    start_values = c_points + prior_fix
    return lax.map(advance, start_values)
```

```python
import functools

import jax
import jax.numpy as jnp
from jax import lax
from jax.experimental import pallas as pl
from jax.experimental.pallas import tpu as pltpu
from jax.sharding import PartitionSpec as P

MESH = pl.DeviceIdType.MESH
f32 = jnp.float32

NEAR = 7
FAR = 6
HD = NEAR + FAR
SC = 1.0 / 128.0
TOL = 1e-7


def loop(lo, hi, body, init, unroll):
    n = hi - lo
    while n % unroll:
        unroll -= 1
    return lax.fori_loop(lo, hi, body, init, unroll=unroll)


def gauss_jordan(m, n):
    rows = lax.broadcasted_iota(jnp.int32, (8, 128), 0)
    first = m
    for k in range(n):
        row = jnp.broadcast_to(m[k : k + 1, :], (8, 128))
        col = jnp.broadcast_to(m[:, k : k + 1], (8, 128))
        pivot = jnp.broadcast_to(row[:, k : k + 1], (8, 128))
        size = jnp.broadcast_to(jnp.broadcast_to(first[k : k + 1, :], (8, 128))[:, k : k + 1], (8, 128))
        good = pivot > TOL * size
        inverse = jnp.where(good, 1.0 / jnp.where(good, pivot, 1.0), 0.0)
        row = row * inverse
        m = jnp.where(rows == k, row, m - col * row)
    return jnp.broadcast_to(m[:, 6:7], (8, 128))


def kernel(ns, nt, nz, cp_hbm, co_hbm, cond_hbm, force_hbm, out_hbm, X, C, F, WZ, WY, WX, E, V, W, CP, CO, CR, O,
           row_buf, gather, load_sem, out_sem, halo_send, halo_recv, shift_send, shift_recv, ar_send, ar_recv):
    ny, nx = X.shape[1:]
    s = lax.axis_index("space")
    t = lax.axis_index("tm")
    a, b = HD, HD + nz
    has_left, has_right = s > 0, s < ns - 1

    loads = [
        pltpu.make_async_copy(co_hbm, CO, load_sem.at[0]),
        pltpu.make_async_copy(cond_hbm, C.at[pl.ds(a, nz)], load_sem.at[1]),
        pltpu.make_async_copy(force_hbm, F.at[pl.ds(a, nz)], load_sem.at[2]),
        pltpu.make_async_copy(cp_hbm, CP, load_sem.at[3]),
    ]
    for c in loads:
        c.start()

    barrier = pltpu.get_barrier_semaphore()
    for d in range(1, ns):
        pl.semaphore_signal(barrier, inc=1, device_id={"space": lax.rem(s + d, ns)}, device_id_type=MESH)

    @pl.when(t > 0)
    def _():
        pl.semaphore_signal(barrier, inc=1, device_id={"tm": lax.rem(t + nt - 1, nt)}, device_id_type=MESH)

    @pl.when(t < nt - 1)
    def _():
        pl.semaphore_signal(barrier, inc=1, device_id={"tm": lax.rem(t + 1, nt)}, device_id_type=MESH)

    zero = jnp.zeros((ny, nx), f32)

    def clear(lo, hi):
        def body(k, carry):
            X[k] = zero
            C[k] = zero
            F[k] = zero
            return carry

        lax.fori_loop(lo, hi, body, 0)

    @pl.when(jnp.logical_not(has_left))
    def _():
        clear(0, a)

    @pl.when(jnp.logical_not(has_right))
    def _():
        clear(b, b + HD)

    @pl.when(t == 0)
    def _():
        def body(k, carry):
            CR[k] = zero
            return carry

        lax.fori_loop(0, nz, body, 0)

    pl.semaphore_wait(barrier, (ns - 1) + (t > 0).astype(jnp.int32) + (t < nt - 1).astype(jnp.int32))

    shift = pltpu.make_async_remote_copy(
        CO, CR, shift_send, shift_recv, device_id={"tm": lax.rem(t + 1, nt)}, device_id_type=MESH
    )

    def halo(field, far, side):
        ref = (X, C, F)[field]
        near = NEAR - 1 if field == 2 else NEAR
        n = FAR if far else near
        if side == 0:
            src = b - near - FAR if far else b - near
            dst = a - near - FAR if far else a - near
            to = lax.rem(s + 1, ns)
        else:
            src = a + near if far else a
            dst = b + near if far else b
            to = lax.rem(s + ns - 1, ns)
        i = field * 4 + far * 2 + side
        return pltpu.make_async_remote_copy(
            ref.at[pl.ds(src, n)], ref.at[pl.ds(dst, n)], halo_send.at[i], halo_recv.at[i],
            device_id={"space": to}, device_id_type=MESH,
        )

    def send_halo(fields, far):
        @pl.when(has_right)
        def _():
            for f in fields:
                halo(f, far, 0).start()

        @pl.when(has_left)
        def _():
            for f in fields:
                halo(f, far, 1).start()

    def wait_halo(fields, far, sent):
        @pl.when(has_right if sent else has_left)
        def _():
            for f in fields:
                c = halo(f, far, 0)
                c.wait_send() if sent else c.wait_recv()

        @pl.when(has_left if sent else has_right)
        def _():
            for f in fields:
                c = halo(f, far, 1)
                c.wait_send() if sent else c.wait_recv()

    loads[0].wait()

    @pl.when(t < nt - 1)
    def _():
        shift.start()

    loads[1].wait()
    loads[2].wait()
    send_halo((1, 2), 0)

    edge_y = lax.broadcasted_iota(jnp.int32, (ny, nx), 0)
    edge_x = lax.broadcasted_iota(jnp.int32, (ny, nx), 1)
    outer = ((edge_y == 0).astype(f32) + (edge_y == ny - 1).astype(f32)
             + (edge_x == 0).astype(f32) + (edge_x == nx - 1).astype(f32))
    keep_y = (edge_y < ny - 1).astype(f32) * (2 * SC)
    keep_x = (edge_x < nx - 1).astype(f32) * (2 * SC)
    outer = outer * (2 * SC)

    def plane_weights(lo, hi):
        def body(k, carry):
            c = C[k]
            WY[k] = keep_y * (c + pltpu.roll(c, ny - 1, 0))
            WX[k] = keep_x * (c + pltpu.roll(c, nx - 1, 1))
            E[k] = SC + outer * c
            return carry

        loop(lo, hi, body, 0, 2)

    def face_weights(lo, hi):
        def body(k, carry):
            WZ[k] = (2 * SC) * (C[k - 1] + C[k])
            return carry

        loop(lo, hi, body, 0, 2)

    def apply(src, dst, lo, hi, finish=None):
        def body(k, below):
            v = src(k)
            above = WZ[k + 1] * (src(k + 1) - v)
            fy = WY[k] * (pltpu.roll(v, ny - 1, 0) - v)
            fx = WX[k] * (pltpu.roll(v, nx - 1, 1) - v)
            out = E[k] * v - ((above - below) + (fy - pltpu.roll(fy, 1, 0)) + (fx - pltpu.roll(fx, 1, 1)))
            dst(k, out, v)
            return above

        loop(lo, hi, body, WZ[lo] * (src(lo) - src(lo - 1)), 2)

    def from_x(k):
        return X[k]

    def start_residual(k, image, v):
        V[0, k] = (v + 0.25 * F[k]) - 128.0 * image

    def power(buf, j, lo, hi):
        def put(k, image, v):
            buf[j, k] = image

        apply(lambda k: buf[j - 1, k], put, lo, hi)

    def dots(pairs, used):
        def body(k, accs):
            val = {u: (V if u[0] == "v" else W)[int(u[1]), k] for u in used}
            out = []
            for acc, (p, q) in zip(accs, pairs):
                z = val[p] * val[q]
                out.append(acc + ((z[0:8] + z[8:16]) + (z[16:24] + z[24:32])))
            return tuple(out)

        return loop(a, b, body, tuple(jnp.zeros((8, nx), f32) for _ in pairs), 2)

    lane = lax.broadcasted_iota(jnp.int32, (1, 128), 1)

    def to_row(pairs, places, accs):
        r = jnp.zeros((1, 128), f32)
        for pair, acc in zip(pairs, accs):
            total = jnp.sum(jnp.sum(acc, axis=0, keepdims=True), axis=1, keepdims=True)
            mask = None
            for i, j in places[pair]:
                m = lane == (j - 8 * i) % 128
                mask = m if mask is None else jnp.logical_or(mask, m)
            r = jnp.where(mask, jnp.broadcast_to(total, (1, 128)), r)
        return r

    def exchange(n, d):
        return pltpu.make_async_remote_copy(
            row_buf.at[n], gather.at[n, s], ar_send.at[n, d - 1], ar_recv.at[n, d - 1],
            device_id={"space": lax.rem(s + d, ns)}, device_id_type=MESH,
        )

    order = sorted(range(1, ns), key=lambda d: -min(d, ns - d))

    def send_row(n, r):
        row_buf[n] = r
        for d in order:
            exchange(n, d).start()

    def total_tile(n, r):
        for d in order:
            exchange(n, d).wait()
        parts = [jnp.where(s == q, r, gather[n, q]) for q in range(ns)]
        while len(parts) > 1:
            parts = [parts[i] + parts[i + 1] for i in range(0, len(parts), 2)]
        return pltpu.roll(jnp.broadcast_to(parts[0], (8, 128)), 0, 1, stride=8, stride_axis=0)

    first_pairs = (("v0", "v0"), ("v0", "v1"), ("v0", "v2"), ("v1", "v1"), ("v1", "v2"), ("v2", "v2"), ("v2", "v3"))
    first_places = {
        ("v0", "v0"): ((0, 6),), ("v0", "v1"): ((0, 0), (1, 6)), ("v0", "v2"): ((2, 6),),
        ("v1", "v1"): ((1, 0), (0, 1)), ("v1", "v2"): ((1, 1), (2, 0), (0, 2)),
        ("v2", "v2"): ((2, 1), (1, 2)), ("v2", "v3"): ((2, 2),),
    }
    second_pairs = [("w0", "v0")] + [(f"w{i}", f"v{j}") for i in range(3) for j in (1, 2, 3)]
    second_places = {("w0", "v0"): ((0, 6),)}
    for i in range(3):
        for j in range(3):
            second_places[(f"w{i}", f"v{j + 1}")] = ((3 + i, j), (j, 3 + i))
    second_places[("w0", "v1")] += ((1, 6),)
    second_places[("w0", "v2")] += ((2, 6),)
    for pair, where in first_places.items():
        q = tuple(p.replace("v", "w") for p in pair)
        second_pairs.append(q)
        second_places[q] = tuple((i + 3, j if j == 6 else j + 3) for i, j in where)

    def spread(y, j):
        return jnp.broadcast_to(y[j : j + 1, :], (ny, nx))

    def next_residual(coefs, lo, hi):
        def body(k, carry):
            W[0, k] = V[0, k] - (coefs[0] * V[1, k] + coefs[1] * V[2, k] + coefs[2] * V[3, k])
            return carry

        loop(lo, hi, body, 0, 2)

    def section(which):
        lo, hi = lambda d: a - d, lambda d: b + d
        apply(from_x, start_residual, lo(6), hi(6))
        for j in (1, 2, 3):
            power(V, j, lo(6 - j), hi(6 - j))
        r = to_row(first_pairs, first_places, dots(first_pairs, ("v0", "v1", "v2", "v3")))
        send_row(2 * which, r)
        tile = total_tile(2 * which, r)
        y1 = gauss_jordan(tile, 3)
        coefs = [spread(y1, j) for j in range(3)]
        next_residual(coefs, lo(3), hi(3))
        for j in (1, 2, 3):
            power(W, j, lo(3 - j), hi(3 - j))
        r = to_row(second_pairs, second_places,
                   dots(second_pairs, ("v0", "v1", "v2", "v3", "w0", "w1", "w2", "w3")))
        send_row(2 * which + 1, r)
        if which == 0:
            wait_halo((1, 2, 0), 1, False)
            plane_weights(a - 12, a - 6)
            plane_weights(b + 6, b + 12)
            face_weights(a - 12, a - 6)
            face_weights(b + 7, b + 13)
            apply(from_x, start_residual, lo(12), lo(6))
            apply(from_x, start_residual, hi(6), hi(12))
            for j in (1, 2, 3):
                power(V, j, lo(12 - j), lo(6 - j))
                power(V, j, hi(6 - j), hi(12 - j))
            next_residual(coefs, lo(9), lo(3))
            next_residual(coefs, hi(3), hi(9))
            for j in (1, 2):
                power(W, j, lo(9 - j), lo(3 - j))
                power(W, j, hi(3 - j), hi(9 - j))
        rows = lax.broadcasted_iota(jnp.int32, (8, 128), 0)
        lanes = lax.broadcasted_iota(jnp.int32, (8, 128), 1)
        old = jnp.logical_and(jnp.logical_and(rows < 3, lanes < 3), rows >= 0)
        tile2 = jnp.where(old, tile, total_tile(2 * which + 1, r))
        y2 = gauss_jordan(tile2, 6)
        both = [(y1 + y2) * SC, y2 * SC]
        cv = [spread(both[0], j) for j in range(3)]
        cw = [spread(both[1], 3 + j) for j in range(3)]

        def result(k):
            v = (cv[0] * V[0, k] + cv[1] * V[1, k]) + cv[2] * V[2, k]
            w = (cw[0] * W[0, k] + cw[1] * W[1, k]) + cw[2] * W[2, k]
            return X[k] + (v + w)

        return result

    loads[3].wait()

    @pl.when(t > 0)
    def _():
        shift.wait_recv()

    def add(k, carry):
        X[a + k] = CP[k] + CR[k]
        return carry

    loop(0, nz, add, 0, 4)
    send_halo((0,), 0)
    send_halo((1, 2, 0), 1)

    wait_halo((1, 2), 0, False)
    plane_weights(a - 6, b + 6)
    face_weights(a - 6, b + 7)

    @pl.when(jnp.logical_not(has_left))
    def _():
        WZ[a] = zero
        E[a] = E[a] + (2 * SC) * C[a]

    @pl.when(jnp.logical_not(has_right))
    def _():
        WZ[b] = zero
        E[b - 1] = E[b - 1] + (2 * SC) * C[b - 1]

    wait_halo((0,), 0, False)

    result = section(0)
    wait_halo((0,), 0, True)
    wait_halo((0,), 1, True)

    def put_x(k, carry):
        X[k] = result(k)
        return carry

    loop(a - 7, b + 7, put_x, 0, 2)
    out0 = pltpu.make_async_copy(X.at[pl.ds(a, nz)], out_hbm.at[0], out_sem.at[0])
    out0.start()
    result = section(1)

    def put_o(k, carry):
        O[k] = result(a + k)
        return carry

    loop(0, nz, put_o, 0, 2)
    out1 = pltpu.make_async_copy(O, out_hbm.at[1], out_sem.at[1])
    out1.start()

    wait_halo((1, 2), 0, True)
    wait_halo((1, 2), 1, True)

    @pl.when(t < nt - 1)
    def _():
        shift.wait_send()

    out0.wait()
    out1.wait()


def solution(mesh):
    ns, nt = mesh.shape["space"], mesh.shape["tm"]

    def body(c_points, corrections, conductivity, forcing):
        nz, ny, nx = conductivity.shape
        ext = nz + 2 * HD
        out = pl.pallas_call(
            functools.partial(kernel, ns, nt, nz),
            out_shape=jax.ShapeDtypeStruct((2, nz, ny, nx), f32),
            in_specs=[pl.BlockSpec(memory_space=pl.ANY)] * 4,
            out_specs=pl.BlockSpec(memory_space=pl.ANY),
            scratch_shapes=[
                pltpu.VMEM((ext, ny, nx), f32),
                pltpu.VMEM((ext, ny, nx), f32),
                pltpu.VMEM((ext, ny, nx), f32),
                pltpu.VMEM((ext + 1, ny, nx), f32),
                pltpu.VMEM((ext, ny, nx), f32),
                pltpu.VMEM((ext, ny, nx), f32),
                pltpu.VMEM((ext, ny, nx), f32),
                pltpu.VMEM((4, ext, ny, nx), f32),
                pltpu.VMEM((4, ext, ny, nx), f32),
                pltpu.VMEM((nz, ny, nx), f32),
                pltpu.VMEM((nz, ny, nx), f32),
                pltpu.VMEM((nz, ny, nx), f32),
                pltpu.VMEM((nz, ny, nx), f32),
                pltpu.VMEM((4, 1, 128), f32),
                pltpu.VMEM((4, ns, 1, 128), f32),
                pltpu.SemaphoreType.DMA((4,)),
                pltpu.SemaphoreType.DMA((2,)),
                pltpu.SemaphoreType.DMA((12,)),
                pltpu.SemaphoreType.DMA((12,)),
                pltpu.SemaphoreType.DMA,
                pltpu.SemaphoreType.DMA,
                pltpu.SemaphoreType.DMA((4, ns - 1)),
                pltpu.SemaphoreType.DMA((4, ns - 1)),
            ],
            compiler_params=pltpu.CompilerParams(collective_id=0, has_side_effects=True),
        )(c_points[0], corrections[0], conductivity, forcing)
        return out[None]

    in_specs = (
        P("tm", "space", None, None),
        P("tm", "space", None, None),
        P("space", None, None),
        P("space", None, None),
    )
    out_specs = P("tm", None, "space", None, None)
    return jax.shard_map(body, mesh=mesh, in_specs=in_specs, out_specs=out_specs, check_vma=False)
```

```python
import functools

import jax
import jax.numpy as jnp
from jax import lax
from jax.experimental import pallas as pl
from jax.experimental.pallas import tpu as pltpu
from jax.sharding import PartitionSpec as P

MESH = pl.DeviceIdType.MESH
f32 = jnp.float32

NEAR = 7
FAR = 6
HD = NEAR + FAR
SC = 1.0 / 128.0
TOL = 1e-7


def loop(lo, hi, body, init, unroll):
    n = hi - lo
    while n % unroll:
        unroll -= 1
    return lax.fori_loop(lo, hi, body, init, unroll=unroll)


def gauss_jordan(m, n):
    rows = lax.broadcasted_iota(jnp.int32, (8, 128), 0)
    first = m
    for k in range(n):
        row = jnp.broadcast_to(m[k : k + 1, :], (8, 128))
        col = jnp.broadcast_to(m[:, k : k + 1], (8, 128))
        pivot = jnp.broadcast_to(row[:, k : k + 1], (8, 128))
        size = jnp.broadcast_to(jnp.broadcast_to(first[k : k + 1, :], (8, 128))[:, k : k + 1], (8, 128))
        good = pivot > TOL * size
        inverse = jnp.where(good, 1.0 / jnp.where(good, pivot, 1.0), 0.0)
        row = row * inverse
        m = jnp.where(rows == k, row, m - col * row)
    return jnp.broadcast_to(m[:, 6:7], (8, 128))


def kernel(ns, nt, nz, cp_hbm, co_hbm, cond_hbm, force_hbm, out_hbm, X, C, F, WZ, WY, WX, E, V, W, CP, CO, CR, O,
           row_buf, gather, load_sem, out_sem, halo_send, halo_recv, shift_send, shift_recv, ar_send, ar_recv):
    ny, nx = X.shape[1:]
    s = lax.axis_index("space")
    t = lax.axis_index("tm")
    a, b = HD, HD + nz
    has_left, has_right = s > 0, s < ns - 1

    loads = [
        pltpu.make_async_copy(co_hbm, CO, load_sem.at[0]),
        pltpu.make_async_copy(cond_hbm, C.at[pl.ds(a, nz)], load_sem.at[1]),
        pltpu.make_async_copy(force_hbm, F.at[pl.ds(a, nz)], load_sem.at[2]),
        pltpu.make_async_copy(cp_hbm, CP, load_sem.at[3]),
    ]
    for c in loads:
        c.start()

    barrier = pltpu.get_barrier_semaphore()
    for d in range(1, ns):
        pl.semaphore_signal(barrier, inc=1, device_id={"space": lax.rem(s + d, ns)}, device_id_type=MESH)

    @pl.when(t > 0)
    def _():
        pl.semaphore_signal(barrier, inc=1, device_id={"tm": lax.rem(t + nt - 1, nt)}, device_id_type=MESH)

    @pl.when(t < nt - 1)
    def _():
        pl.semaphore_signal(barrier, inc=1, device_id={"tm": lax.rem(t + 1, nt)}, device_id_type=MESH)

    zero = jnp.zeros((ny, nx), f32)

    def clear(lo, hi):
        def body(k, carry):
            X[k] = zero
            C[k] = zero
            F[k] = zero
            return carry

        lax.fori_loop(lo, hi, body, 0)

    @pl.when(jnp.logical_not(has_left))
    def _():
        clear(0, a)

    @pl.when(jnp.logical_not(has_right))
    def _():
        clear(b, b + HD)

    @pl.when(t == 0)
    def _():
        def body(k, carry):
            CR[k] = zero
            return carry

        lax.fori_loop(0, nz, body, 0)

    pl.semaphore_wait(barrier, (ns - 1) + (t > 0).astype(jnp.int32) + (t < nt - 1).astype(jnp.int32))

    shift = pltpu.make_async_remote_copy(
        CO, CR, shift_send, shift_recv, device_id={"tm": lax.rem(t + 1, nt)}, device_id_type=MESH
    )

    def halo(field, far, side):
        ref = (X, C, F)[field]
        near = NEAR - 1 if field == 2 else NEAR
        n = FAR if far else near
        if side == 0:
            src = b - near - FAR if far else b - near
            dst = a - near - FAR if far else a - near
            to = lax.rem(s + 1, ns)
        else:
            src = a + near if far else a
            dst = b + near if far else b
            to = lax.rem(s + ns - 1, ns)
        i = field * 4 + far * 2 + side
        return pltpu.make_async_remote_copy(
            ref.at[pl.ds(src, n)], ref.at[pl.ds(dst, n)], halo_send.at[i], halo_recv.at[i],
            device_id={"space": to}, device_id_type=MESH,
        )

    def send_halo(fields, far):
        @pl.when(has_right)
        def _():
            for f in fields:
                halo(f, far, 0).start()

        @pl.when(has_left)
        def _():
            for f in fields:
                halo(f, far, 1).start()

    def wait_halo(fields, far, sent):
        @pl.when(has_right if sent else has_left)
        def _():
            for f in fields:
                c = halo(f, far, 0)
                c.wait_send() if sent else c.wait_recv()

        @pl.when(has_left if sent else has_right)
        def _():
            for f in fields:
                c = halo(f, far, 1)
                c.wait_send() if sent else c.wait_recv()

    loads[0].wait()

    @pl.when(t < nt - 1)
    def _():
        shift.start()

    loads[1].wait()
    loads[2].wait()
    send_halo((1, 2), 0)

    edge_y = lax.broadcasted_iota(jnp.int32, (ny, nx), 0)
    edge_x = lax.broadcasted_iota(jnp.int32, (ny, nx), 1)
    outer = ((edge_y == 0).astype(f32) + (edge_y == ny - 1).astype(f32)
             + (edge_x == 0).astype(f32) + (edge_x == nx - 1).astype(f32))
    keep_y = (edge_y < ny - 1).astype(f32) * (2 * SC)
    keep_x = (edge_x < nx - 1).astype(f32) * (2 * SC)
    outer = outer * (2 * SC)

    def plane_weights(lo, hi):
        def body(k, carry):
            c = C[k]
            WY[k] = keep_y * (c + pltpu.roll(c, ny - 1, 0))
            WX[k] = keep_x * (c + pltpu.roll(c, nx - 1, 1))
            E[k] = SC + outer * c
            return carry

        loop(lo, hi, body, 0, 2)

    def face_weights(lo, hi):
        def body(k, carry):
            WZ[k] = (2 * SC) * (C[k - 1] + C[k])
            return carry

        loop(lo, hi, body, 0, 2)

    def apply(src, dst, lo, hi, finish=None):
        def body(k, below):
            v = src(k)
            above = WZ[k + 1] * (src(k + 1) - v)
            fy = WY[k] * (pltpu.roll(v, ny - 1, 0) - v)
            fx = WX[k] * (pltpu.roll(v, nx - 1, 1) - v)
            out = E[k] * v - ((above - below) + (fy - pltpu.roll(fy, 1, 0)) + (fx - pltpu.roll(fx, 1, 1)))
            dst(k, out, v)
            return above

        loop(lo, hi, body, WZ[lo] * (src(lo) - src(lo - 1)), 2)

    def from_x(k):
        return X[k]

    def start_residual(k, image, v):
        V[0, k] = (v + 0.25 * F[k]) - 128.0 * image

    def power(buf, j, lo, hi):
        def put(k, image, v):
            buf[j, k] = image

        apply(lambda k: buf[j - 1, k], put, lo, hi)

    def dots(pairs, used):
        def body(k, accs):
            val = {u: (V if u[0] == "v" else W)[int(u[1]), k] for u in used}
            out = []
            for acc, (p, q) in zip(accs, pairs):
                z = val[p] * val[q]
                out.append(acc + ((z[0:8] + z[8:16]) + (z[16:24] + z[24:32])))
            return tuple(out)

        return loop(a, b, body, tuple(jnp.zeros((8, nx), f32) for _ in pairs), 2)

    lane = lax.broadcasted_iota(jnp.int32, (1, 128), 1)

    def to_row(pairs, places, accs):
        r = jnp.zeros((1, 128), f32)
        for pair, acc in zip(pairs, accs):
            total = jnp.sum(jnp.sum(acc, axis=0, keepdims=True), axis=1, keepdims=True)
            mask = None
            for i, j in places[pair]:
                m = lane == (j - 8 * i) % 128
                mask = m if mask is None else jnp.logical_or(mask, m)
            r = jnp.where(mask, jnp.broadcast_to(total, (1, 128)), r)
        return r

    def exchange(n, d):
        return pltpu.make_async_remote_copy(
            row_buf.at[n], gather.at[n, s], ar_send.at[n, d - 1], ar_recv.at[n, d - 1],
            device_id={"space": lax.rem(s + d, ns)}, device_id_type=MESH,
        )

    order = sorted(range(1, ns), key=lambda d: -min(d, ns - d))

    def send_row(n, r):
        row_buf[n] = r
        for d in order:
            exchange(n, d).start()

    def total_tile(n, r):
        for d in order:
            exchange(n, d).wait()
        parts = [jnp.where(s == q, r, gather[n, q]) for q in range(ns)]
        while len(parts) > 1:
            parts = [parts[i] + parts[i + 1] for i in range(0, len(parts), 2)]
        return pltpu.roll(jnp.broadcast_to(parts[0], (8, 128)), 0, 1, stride=8, stride_axis=0)

    first_pairs = (("v0", "v0"), ("v0", "v1"), ("v0", "v2"), ("v1", "v1"), ("v1", "v2"), ("v2", "v2"), ("v2", "v3"))
    first_places = {
        ("v0", "v0"): ((0, 6),), ("v0", "v1"): ((0, 0), (1, 6)), ("v0", "v2"): ((2, 6),),
        ("v1", "v1"): ((1, 0), (0, 1)), ("v1", "v2"): ((1, 1), (2, 0), (0, 2)),
        ("v2", "v2"): ((2, 1), (1, 2)), ("v2", "v3"): ((2, 2),),
    }
    second_pairs = [("w0", "v0")] + [(f"w{i}", f"v{j}") for i in range(3) for j in (1, 2, 3)]
    second_places = {("w0", "v0"): ((0, 6),)}
    for i in range(3):
        for j in range(3):
            second_places[(f"w{i}", f"v{j + 1}")] = ((3 + i, j), (j, 3 + i))
    second_places[("w0", "v1")] += ((1, 6),)
    second_places[("w0", "v2")] += ((2, 6),)
    for pair, where in first_places.items():
        q = tuple(p.replace("v", "w") for p in pair)
        second_pairs.append(q)
        second_places[q] = tuple((i + 3, j if j == 6 else j + 3) for i, j in where)

    def spread(y, j):
        return jnp.broadcast_to(y[j : j + 1, :], (ny, nx))

    def next_residual(coefs, lo, hi):
        def body(k, carry):
            W[0, k] = V[0, k] - (coefs[0] * V[1, k] + coefs[1] * V[2, k] + coefs[2] * V[3, k])
            return carry

        loop(lo, hi, body, 0, 2)

    def section(which):
        lo, hi = lambda d: a - d, lambda d: b + d
        apply(from_x, start_residual, lo(6), hi(6))
        for j in (1, 2, 3):
            power(V, j, lo(6 - j), hi(6 - j))
        r = to_row(first_pairs, first_places, dots(first_pairs, ("v0", "v1", "v2", "v3")))
        send_row(2 * which, r)
        if which == 0:
            send_halo((1, 2, 0), 1)
        tile = total_tile(2 * which, r)
        y1 = gauss_jordan(tile, 3)
        coefs = [spread(y1, j) for j in range(3)]
        next_residual(coefs, lo(3), hi(3))
        for j in (1, 2, 3):
            power(W, j, lo(3 - j), hi(3 - j))
        r = to_row(second_pairs, second_places,
                   dots(second_pairs, ("v0", "v1", "v2", "v3", "w0", "w1", "w2", "w3")))
        send_row(2 * which + 1, r)
        if which == 0:
            wait_halo((1, 2, 0), 1, False)
            plane_weights(a - 12, a - 6)
            plane_weights(b + 6, b + 12)
            face_weights(a - 12, a - 6)
            face_weights(b + 7, b + 13)
            apply(from_x, start_residual, lo(12), lo(6))
            apply(from_x, start_residual, hi(6), hi(12))
            for j in (1, 2, 3):
                power(V, j, lo(12 - j), lo(6 - j))
                power(V, j, hi(6 - j), hi(12 - j))
            next_residual(coefs, lo(9), lo(3))
            next_residual(coefs, hi(3), hi(9))
            for j in (1, 2):
                power(W, j, lo(9 - j), lo(3 - j))
                power(W, j, hi(3 - j), hi(9 - j))
        rows = lax.broadcasted_iota(jnp.int32, (8, 128), 0)
        lanes = lax.broadcasted_iota(jnp.int32, (8, 128), 1)
        old = jnp.logical_and(jnp.logical_and(rows < 3, lanes < 3), rows >= 0)
        tile2 = jnp.where(old, tile, total_tile(2 * which + 1, r))
        y2 = gauss_jordan(tile2, 6)
        both = [(y1 + y2) * SC, y2 * SC]
        cv = [spread(both[0], j) for j in range(3)]
        cw = [spread(both[1], 3 + j) for j in range(3)]

        def result(k):
            v = (cv[0] * V[0, k] + cv[1] * V[1, k]) + cv[2] * V[2, k]
            w = (cw[0] * W[0, k] + cw[1] * W[1, k]) + cw[2] * W[2, k]
            return X[k] + (v + w)

        return result

    loads[3].wait()

    @pl.when(t > 0)
    def _():
        shift.wait_recv()

    def add(k, carry):
        X[a + k] = CP[k] + CR[k]
        return carry

    loop(0, nz, add, 0, 4)
    send_halo((0,), 0)

    wait_halo((1, 2), 0, False)
    plane_weights(a - 6, b + 6)
    face_weights(a - 6, b + 7)

    @pl.when(jnp.logical_not(has_left))
    def _():
        WZ[a] = zero
        E[a] = E[a] + (2 * SC) * C[a]

    @pl.when(jnp.logical_not(has_right))
    def _():
        WZ[b] = zero
        E[b - 1] = E[b - 1] + (2 * SC) * C[b - 1]

    wait_halo((0,), 0, False)

    result = section(0)
    wait_halo((0,), 0, True)
    wait_halo((0,), 1, True)

    def put_x(k, carry):
        X[k] = result(k)
        return carry

    loop(a - 7, b + 7, put_x, 0, 2)
    out0 = pltpu.make_async_copy(X.at[pl.ds(a, nz)], out_hbm.at[0], out_sem.at[0])
    out0.start()
    result = section(1)

    def put_o(k, carry):
        O[k] = result(a + k)
        return carry

    loop(0, nz, put_o, 0, 2)
    out1 = pltpu.make_async_copy(O, out_hbm.at[1], out_sem.at[1])
    out1.start()

    wait_halo((1, 2), 0, True)
    wait_halo((1, 2), 1, True)

    @pl.when(t < nt - 1)
    def _():
        shift.wait_send()

    out0.wait()
    out1.wait()


def solution(mesh):
    ns, nt = mesh.shape["space"], mesh.shape["tm"]

    def body(c_points, corrections, conductivity, forcing):
        nz, ny, nx = conductivity.shape
        ext = nz + 2 * HD
        out = pl.pallas_call(
            functools.partial(kernel, ns, nt, nz),
            out_shape=jax.ShapeDtypeStruct((2, nz, ny, nx), f32),
            in_specs=[pl.BlockSpec(memory_space=pl.ANY)] * 4,
            out_specs=pl.BlockSpec(memory_space=pl.ANY),
            scratch_shapes=[
                pltpu.VMEM((ext, ny, nx), f32),
                pltpu.VMEM((ext, ny, nx), f32),
                pltpu.VMEM((ext, ny, nx), f32),
                pltpu.VMEM((ext + 1, ny, nx), f32),
                pltpu.VMEM((ext, ny, nx), f32),
                pltpu.VMEM((ext, ny, nx), f32),
                pltpu.VMEM((ext, ny, nx), f32),
                pltpu.VMEM((4, ext, ny, nx), f32),
                pltpu.VMEM((4, ext, ny, nx), f32),
                pltpu.VMEM((nz, ny, nx), f32),
                pltpu.VMEM((nz, ny, nx), f32),
                pltpu.VMEM((nz, ny, nx), f32),
                pltpu.VMEM((nz, ny, nx), f32),
                pltpu.VMEM((4, 1, 128), f32),
                pltpu.VMEM((4, ns, 1, 128), f32),
                pltpu.SemaphoreType.DMA((4,)),
                pltpu.SemaphoreType.DMA((2,)),
                pltpu.SemaphoreType.DMA((12,)),
                pltpu.SemaphoreType.DMA((12,)),
                pltpu.SemaphoreType.DMA,
                pltpu.SemaphoreType.DMA,
                pltpu.SemaphoreType.DMA((4, ns - 1)),
                pltpu.SemaphoreType.DMA((4, ns - 1)),
            ],
            compiler_params=pltpu.CompilerParams(collective_id=0, has_side_effects=True),
        )(c_points[0], corrections[0], conductivity, forcing)
        return out[None]

    in_specs = (
        P("tm", "space", None, None),
        P("tm", "space", None, None),
        P("space", None, None),
        P("space", None, None),
    )
    out_specs = P("tm", None, "space", None, None)
    return jax.shard_map(body, mesh=mesh, in_specs=in_specs, out_specs=out_specs, check_vma=False)
```

```python
import functools

import jax
import jax.numpy as jnp
from jax import lax
from jax.experimental import pallas as pl
from jax.experimental.pallas import tpu as pltpu
from jax.sharding import PartitionSpec as P

MESH = pl.DeviceIdType.MESH
f32 = jnp.float32

LEVELS = ((0, 4), (4, 7), (7, 13))
FORCE_LEVELS = ((0, 3), (3, 6), (6, 12))
HD = 13
SHARE = 4
ALONG_Z = 4
SC = 1.0 / 128.0
TOL = 1e-7
APPLY = 28


def loop(lo, hi, body, init, unroll):
    n = hi - lo
    if n <= unroll:
        return lax.fori_loop(lo, hi, body, init, unroll=n)
    rest = n % unroll
    init = lax.fori_loop(lo, hi - rest, body, init, unroll=unroll)
    return lax.fori_loop(hi - rest, hi, body, init, unroll=rest) if rest else init


def gauss_jordan(m, n):
    rows = lax.broadcasted_iota(jnp.int32, (8, 128), 0)
    first = m
    for k in range(n):
        row = jnp.broadcast_to(m[k : k + 1, :], (8, 128))
        col = jnp.broadcast_to(m[:, k : k + 1], (8, 128))
        pivot = jnp.broadcast_to(row[:, k : k + 1], (8, 128))
        size = jnp.broadcast_to(jnp.broadcast_to(first[k : k + 1, :], (8, 128))[:, k : k + 1], (8, 128))
        good = pivot > TOL * size
        inverse = jnp.where(good, 1.0 / jnp.where(good, pivot, 1.0), 0.0)
        row = row * inverse
        m = jnp.where(rows == k, row, m - col * row)
    return jnp.broadcast_to(m[:, 6:7], (8, 128))


def kernel(ns, nt, nz, cp_hbm, co_hbm, cond_hbm, force_hbm, out_hbm, X, C, F, WZ, WY, WX, WL, E, V, W, CP, CO, CR, O,
           row_buf, gather, load_sem, out_sem, halo_send, halo_recv, chip_send, chip_recv, far_send, far_recv, share_send, share_recv, shift_send, shift_recv, ar_send, ar_recv):
    ny, nx = X.shape[1:]
    s = lax.axis_index("space")
    t = lax.axis_index("tm")
    a, b = HD, HD + nz
    has_left, has_right = s > 0, s < ns - 1

    loads = [
        pltpu.make_async_copy(co_hbm, CO, load_sem.at[0]),
        pltpu.make_async_copy(cond_hbm, C.at[pl.ds(a, nz)], load_sem.at[1]),
        pltpu.make_async_copy(force_hbm, F.at[pl.ds(a, nz)], load_sem.at[2]),
        pltpu.make_async_copy(cp_hbm, CP, load_sem.at[3]),
    ]
    for c in loads:
        c.start()

    barrier = pltpu.get_barrier_semaphore()
    for d in range(1, ns):
        pl.semaphore_signal(barrier, inc=1, device_id={"space": lax.rem(s + d, ns)}, device_id_type=MESH)

    @pl.when(t > 0)
    def _():
        pl.semaphore_signal(barrier, inc=1, device_id={"tm": lax.rem(t + nt - 1, nt)}, device_id_type=MESH)

    @pl.when(t < nt - 1)
    def _():
        pl.semaphore_signal(barrier, inc=1, device_id={"tm": lax.rem(t + 1, nt)}, device_id_type=MESH)

    quarter = t // ALONG_Z

    def sharer(d):
        first = quarter - lax.rem(quarter, SHARE)
        return (first + lax.rem(quarter + d, SHARE)) * ALONG_Z + lax.rem(t, ALONG_Z)

    for d in range(1, SHARE):
        pl.semaphore_signal(barrier, inc=1, device_id={"tm": sharer(d)}, device_id_type=MESH)

    zero = jnp.zeros((ny, nx), f32)

    def clear(lo, hi):
        def body(k, carry):
            X[k] = zero
            C[k] = zero
            F[k] = zero
            return carry

        lax.fori_loop(lo, hi, body, 0)

    @pl.when(jnp.logical_not(has_left))
    def _():
        clear(0, a)

    @pl.when(jnp.logical_not(has_right))
    def _():
        clear(b, b + HD)

    @pl.when(t == 0)
    def _():
        def body(k, carry):
            CR[k] = zero
            return carry

        lax.fori_loop(0, nz, body, 0)

    pl.semaphore_wait(barrier, (ns - 1) + (SHARE - 1) + (t > 0).astype(jnp.int32) + (t < nt - 1).astype(jnp.int32))

    edge = LEVELS[0][1]
    pieces = ((0, edge), (nz - edge, edge), (edge, nz - 2 * edge))

    def shift(i):
        p = pl.ds(*pieces[i])
        return pltpu.make_async_remote_copy(
            CO.at[p], CR.at[p], shift_send.at[i], shift_recv.at[i],
            device_id={"tm": lax.rem(t + 1, nt)}, device_id_type=MESH,
        )

    def halo(level, side):
        d0, d1 = LEVELS[level]
        if side == 0:
            src, dst, to = b - d1, a - d1, lax.rem(s + 1, ns)
        else:
            src, dst, to = a + d0, b + d0, lax.rem(s + ns - 1, ns)
        i = level * 2 + side
        return pltpu.make_async_remote_copy(
            X.at[pl.ds(src, d1 - d0)], X.at[pl.ds(dst, d1 - d0)], halo_send.at[i], halo_recv.at[i],
            device_id={"space": to}, device_id_type=MESH,
        )

    def send_halo(level):
        @pl.when(has_right)
        def _():
            halo(level, 0).start()

        @pl.when(has_left)
        def _():
            halo(level, 1).start()

    def wait_halo(level, sent):
        @pl.when(has_right if sent else has_left)
        def _():
            c = halo(level, 0)
            c.wait_send() if sent else c.wait_recv()

        @pl.when(has_left if sent else has_right)
        def _():
            c = halo(level, 1)
            c.wait_send() if sent else c.wait_recv()

    odd = lax.rem(s, 2)
    outside = jnp.logical_and(has_left, has_right)
    depths = ((LEVELS[0], (LEVELS[1][0], LEVELS[2][1])), (FORCE_LEVELS[0], (FORCE_LEVELS[1][0], FORCE_LEVELS[2][1])))
    my_rows = pl.ds(pl.multiple_of(lax.rem(quarter, SHARE) * (ny // SHARE), 8), ny // SHARE)

    def chip_copy(field, part):
        d0, d1 = depths[field][part]
        ref = (C, F)[field]
        src = odd * (a + d0) + (1 - odd) * (b - d1)
        dst = odd * (b + d0) + (1 - odd) * (a - d1)
        i = field * 2 + part
        return pltpu.make_async_remote_copy(
            ref.at[pl.ds(src, d1 - d0)], ref.at[pl.ds(dst, d1 - d0)], chip_send.at[i], chip_recv.at[i],
            device_id={"space": s + 1 - 2 * odd}, device_id_type=MESH,
        )

    def far_copy(field, part):
        d0, d1 = depths[field][part]
        ref = (C, F)[field]
        src = odd * (b - d1) + (1 - odd) * (a + d0)
        dst = odd * (a - d1) + (1 - odd) * (b + d0)
        i = field * 2 + part
        return pltpu.make_async_remote_copy(
            ref.at[pl.ds(src, d1 - d0), my_rows], ref.at[pl.ds(dst, d1 - d0), my_rows], far_send.at[i], far_recv.at[i],
            device_id={"space": lax.rem(s + ns - 1 + 2 * odd, ns)}, device_id_type=MESH,
        )

    def share_copy(field, part, d):
        d0, d1 = depths[field][part]
        ref = (C, F)[field]
        here = odd * (b + d0) + (1 - odd) * (a - d1)
        p = ref.at[pl.ds(here, d1 - d0), my_rows]
        i = (field * 2 + part) * (SHARE - 1) + d - 1
        return pltpu.make_async_remote_copy(
            p, p, share_send.at[i], share_recv.at[i], device_id={"tm": sharer(d)}, device_id_type=MESH
        )

    def send_inputs(part):
        for f in range(2):
            chip_copy(f, part).start()

        @pl.when(outside)
        def _():
            for f in range(2):
                far_copy(f, part).start()

    def pass_inputs(part):
        @pl.when(outside)
        def _():
            for f in range(2):
                far_copy(f, part).wait_recv()
                for d in range(1, SHARE):
                    share_copy(f, part, d).start()

    def wait_inputs(part):
        for f in range(2):
            chip_copy(f, part).wait_recv()

        @pl.when(outside)
        def _():
            for f in range(2):
                for d in range(1, SHARE):
                    share_copy(f, part, d).wait_recv()

    def wait_inputs_sent():
        for part in range(2):
            for f in range(2):
                chip_copy(f, part).wait_send()

        @pl.when(outside)
        def _():
            for part in range(2):
                for f in range(2):
                    far_copy(f, part).wait_send()
                    for d in range(1, SHARE):
                        share_copy(f, part, d).wait_send()

    loads[1].wait()
    loads[2].wait()
    send_inputs(0)
    loads[0].wait()

    @pl.when(t < nt - 1)
    def _():
        for i in range(3):
            shift(i).start()

    send_inputs(1)

    edge_y = lax.broadcasted_iota(jnp.int32, (ny, nx), 0)
    edge_x = lax.broadcasted_iota(jnp.int32, (ny, nx), 1)
    outer = ((edge_y == 0).astype(f32) + (edge_y == ny - 1).astype(f32)
             + (edge_x == 0).astype(f32) + (edge_x == nx - 1).astype(f32))
    keep_y = (edge_y < ny - 1).astype(f32) * (2 * SC)
    keep_x = (edge_x < nx - 1).astype(f32) * (2 * SC)
    keep_l = (edge_x > 0).astype(f32) * (2 * SC)
    outer = outer * (2 * SC)

    def plane_weights(lo, hi):
        def body(k, carry):
            c = C[k]
            WY[k] = keep_y * (c + pltpu.roll(c, ny - 1, 0))
            WX[k] = keep_x * (c + pltpu.roll(c, nx - 1, 1))
            WL[k] = keep_l * (c + pltpu.roll(c, 1, 1))
            E[k] = SC + outer * c
            return carry

        loop(lo, hi, body, 0, 6)

    def face_weights(lo, hi):
        def body(k, carry):
            WZ[k] = (2 * SC) * (C[k - 1] + C[k])
            return carry

        loop(lo, hi, body, 0, 2)

    def apply(src, dst, lo, hi, finish=None):
        def body(k, below):
            v = src(k)
            above = WZ[k + 1] * (src(k + 1) - v)
            fy = WY[k] * (pltpu.roll(v, ny - 1, 0) - v)
            fx = WX[k] * (pltpu.roll(v, nx - 1, 1) - v) + WL[k] * (pltpu.roll(v, 1, 1) - v)
            out = E[k] * v - ((above - below) + (fy - pltpu.roll(fy, 1, 0)) + fx)
            dst(k, out, v)
            return above

        loop(lo, hi, body, WZ[lo] * (src(lo) - src(lo - 1)), APPLY)

    def from_x(k):
        return X[k]

    def start_residual(k, image, v):
        V[0, k] = (v + 0.25 * F[k]) - 128.0 * image

    def power(buf, j, lo, hi):
        def put(k, image, v):
            buf[j, k] = image

        apply(lambda k: buf[j - 1, k], put, lo, hi)

    def dots(pairs, used):
        def body(k, accs):
            val = {u: (V if u[0] == "v" else W)[int(u[1]), k] for u in used}
            out = []
            for acc, (p, q) in zip(accs, pairs):
                z = val[p] * val[q]
                out.append(acc + ((z[0:8] + z[8:16]) + (z[16:24] + z[24:32])))
            return tuple(out)

        return loop(a, b, body, tuple(jnp.zeros((8, nx), f32) for _ in pairs), 2)

    lane = lax.broadcasted_iota(jnp.int32, (1, 128), 1)

    def to_row(pairs, places, accs):
        r = jnp.zeros((1, 128), f32)
        for pair, acc in zip(pairs, accs):
            total = jnp.sum(jnp.sum(acc, axis=0, keepdims=True), axis=1, keepdims=True)
            mask = None
            for i, j in places[pair]:
                m = lane == (j - 8 * i) % 128
                mask = m if mask is None else jnp.logical_or(mask, m)
            r = jnp.where(mask, jnp.broadcast_to(total, (1, 128)), r)
        return r

    def exchange(n, d):
        return pltpu.make_async_remote_copy(
            row_buf.at[n], gather.at[n, s], ar_send.at[n, d - 1], ar_recv.at[n, d - 1],
            device_id={"space": lax.rem(s + d, ns)}, device_id_type=MESH,
        )

    order = sorted(range(1, ns), key=lambda d: -min(d, ns - d))

    def send_row(n, r):
        row_buf[n] = r
        for d in order:
            exchange(n, d).start()

    def total_tile(n, r):
        for d in order:
            exchange(n, d).wait()
        parts = [jnp.where(s == q, r, gather[n, q]) for q in range(ns)]
        while len(parts) > 1:
            parts = [parts[i] + parts[i + 1] for i in range(0, len(parts), 2)]
        return pltpu.roll(jnp.broadcast_to(parts[0], (8, 128)), 0, 1, stride=8, stride_axis=0)

    first_pairs = (("v0", "v0"), ("v0", "v1"), ("v0", "v2"), ("v1", "v1"), ("v1", "v2"), ("v2", "v2"), ("v2", "v3"))
    first_places = {
        ("v0", "v0"): ((0, 6),), ("v0", "v1"): ((0, 0), (1, 6)), ("v0", "v2"): ((2, 6),),
        ("v1", "v1"): ((1, 0), (0, 1)), ("v1", "v2"): ((1, 1), (2, 0), (0, 2)),
        ("v2", "v2"): ((2, 1), (1, 2)), ("v2", "v3"): ((2, 2),),
    }
    second_pairs = [("w0", "v0")] + [(f"w{i}", f"v{j}") for i in range(3) for j in (1, 2, 3)]
    second_places = {("w0", "v0"): ((0, 6),)}
    for i in range(3):
        for j in range(3):
            second_places[(f"w{i}", f"v{j + 1}")] = ((3 + i, j), (j, 3 + i))
    second_places[("w0", "v1")] += ((1, 6),)
    second_places[("w0", "v2")] += ((2, 6),)
    for pair, where in first_places.items():
        q = tuple(p.replace("v", "w") for p in pair)
        second_pairs.append(q)
        second_places[q] = tuple((i + 3, j if j == 6 else j + 3) for i, j in where)

    def spread(y, j):
        return jnp.broadcast_to(y[j : j + 1, :], (ny, nx))

    def next_residual(coefs, lo, hi):
        def body(k, carry):
            W[0, k] = V[0, k] - (coefs[0] * V[1, k] + coefs[1] * V[2, k] + coefs[2] * V[3, k])
            return carry

        loop(lo, hi, body, 0, 2)

    def both_sides(f, d0, d1):
        f(a - d1, a - d0)
        f(b + d0, b + d1)

    def more_weights(d0, d1):
        both_sides(plane_weights, d0, d1)
        face_weights(a - d1, a - d0)
        face_weights(b + d0 + 1, b + d1 + 1)

    def residual(lo, hi):
        apply(from_x, start_residual, lo, hi)

    def powers(buf, d0, d1, last):
        for j in range(1, last + 1):
            both_sides(functools.partial(power, buf, j), d0 - j, d1 - j)

    def section(which, before=None):
        residual(a - 3, b + 3)
        for j in (1, 2, 3):
            power(V, j, a - 3 + j, b + 3 - j)
        r = to_row(first_pairs, first_places, dots(first_pairs, ("v0", "v1", "v2", "v3")))
        send_row(2 * which, r)
        if which == 0:
            send_halo(2)
            wait_inputs(1)
            wait_halo(1, False)
            more_weights(3, 6)
        else:
            before()
        both_sides(residual, 3, 6)
        powers(V, 3, 6, 3)
        tile = total_tile(2 * which, r)
        y1 = gauss_jordan(tile, 3)
        coefs = [spread(y1, j) for j in range(3)]
        next_residual(coefs, a - 3, b + 3)
        for j in (1, 2, 3):
            power(W, j, a - 3 + j, b + 3 - j)
        r = to_row(second_pairs, second_places,
                   dots(second_pairs, ("v0", "v1", "v2", "v3", "w0", "w1", "w2", "w3")))
        send_row(2 * which + 1, r)
        if which == 0:
            wait_halo(2, False)
            more_weights(6, 12)
            both_sides(residual, 6, 12)
            powers(V, 6, 12, 3)
            both_sides(functools.partial(next_residual, coefs), 3, 9)
            powers(W, 3, 9, 2)
        rows = lax.broadcasted_iota(jnp.int32, (8, 128), 0)
        lanes = lax.broadcasted_iota(jnp.int32, (8, 128), 1)
        old = jnp.logical_and(jnp.logical_and(rows < 3, lanes < 3), rows >= 0)
        tile2 = jnp.where(old, tile, total_tile(2 * which + 1, r))
        y2 = gauss_jordan(tile2, 6)
        both = [(y1 + y2) * SC, y2 * SC]
        cv = [spread(both[0], j) for j in range(3)]
        cw = [spread(both[1], 3 + j) for j in range(3)]

        def result(k):
            v = (cv[0] * V[0, k] + cv[1] * V[1, k]) + cv[2] * V[2, k]
            w = (cw[0] * W[0, k] + cw[1] * W[1, k]) + cw[2] * W[2, k]
            return X[k] + (v + w)

        return result

    loads[3].wait()

    def add(k, carry):
        X[a + k] = CP[k] + CR[k]
        return carry

    def arrive(i):
        @pl.when(t > 0)
        def _():
            shift(i).wait_recv()

        loop(pieces[i][0], sum(pieces[i]), add, 0, 4)

    pass_inputs(0)
    arrive(0)
    arrive(1)
    send_halo(0)
    arrive(2)
    send_halo(1)
    pass_inputs(1)

    wait_inputs(0)
    plane_weights(a - 3, b + 3)
    face_weights(a - 3, b + 4)

    @pl.when(jnp.logical_not(has_left))
    def _():
        WZ[a] = zero
        E[a] = E[a] + (2 * SC) * C[a]

    @pl.when(jnp.logical_not(has_right))
    def _():
        WZ[b] = zero
        E[b - 1] = E[b - 1] + (2 * SC) * C[b - 1]

    wait_halo(0, False)

    result = section(0)
    for level in range(3):
        wait_halo(level, True)

    def put_x(k, carry):
        X[k] = result0(k)
        return carry

    result0 = result
    loop(a - 4, b + 4, put_x, 0, 4)
    out0 = pltpu.make_async_copy(X.at[pl.ds(a, nz)], out_hbm.at[0], out_sem.at[0])
    out0.start()
    result = section(1, lambda: both_sides(lambda lo, hi: loop(lo, hi, put_x, 0, 3), 4, 7))

    def put_o(k, carry):
        O[k] = result(a + k)
        return carry

    loop(0, nz, put_o, 0, 4)
    out1 = pltpu.make_async_copy(O, out_hbm.at[1], out_sem.at[1])
    out1.start()

    wait_inputs_sent()

    @pl.when(t < nt - 1)
    def _():
        for i in range(3):
            shift(i).wait_send()

    out0.wait()
    out1.wait()


def solution(mesh):
    ns, nt = mesh.shape["space"], mesh.shape["tm"]

    def body(c_points, corrections, conductivity, forcing):
        nz, ny, nx = conductivity.shape
        ext = nz + 2 * HD
        out = pl.pallas_call(
            functools.partial(kernel, ns, nt, nz),
            out_shape=jax.ShapeDtypeStruct((2, nz, ny, nx), f32),
            in_specs=[pl.BlockSpec(memory_space=pl.ANY)] * 4,
            out_specs=pl.BlockSpec(memory_space=pl.ANY),
            scratch_shapes=[
                pltpu.VMEM((ext, ny, nx), f32),
                pltpu.VMEM((ext, ny, nx), f32),
                pltpu.VMEM((ext, ny, nx), f32),
                pltpu.VMEM((ext + 1, ny, nx), f32),
                pltpu.VMEM((ext, ny, nx), f32),
                pltpu.VMEM((ext, ny, nx), f32),
                pltpu.VMEM((ext, ny, nx), f32),
                pltpu.VMEM((ext, ny, nx), f32),
                pltpu.VMEM((4, ext, ny, nx), f32),
                pltpu.VMEM((4, ext, ny, nx), f32),
                pltpu.VMEM((nz, ny, nx), f32),
                pltpu.VMEM((nz, ny, nx), f32),
                pltpu.VMEM((nz, ny, nx), f32),
                pltpu.VMEM((nz, ny, nx), f32),
                pltpu.VMEM((4, 1, 128), f32),
                pltpu.VMEM((4, ns, 1, 128), f32),
                pltpu.SemaphoreType.DMA((4,)),
                pltpu.SemaphoreType.DMA((2,)),
                pltpu.SemaphoreType.DMA((6,)),
                pltpu.SemaphoreType.DMA((6,)),
                pltpu.SemaphoreType.DMA((4,)),
                pltpu.SemaphoreType.DMA((4,)),
                pltpu.SemaphoreType.DMA((4,)),
                pltpu.SemaphoreType.DMA((4,)),
                pltpu.SemaphoreType.DMA((4 * (SHARE - 1),)),
                pltpu.SemaphoreType.DMA((4 * (SHARE - 1),)),
                pltpu.SemaphoreType.DMA((3,)),
                pltpu.SemaphoreType.DMA((3,)),
                pltpu.SemaphoreType.DMA((4, ns - 1)),
                pltpu.SemaphoreType.DMA((4, ns - 1)),
            ],
            compiler_params=pltpu.CompilerParams(collective_id=0, has_side_effects=True),
        )(c_points[0], corrections[0], conductivity, forcing)
        return out[None]

    in_specs = (
        P("tm", "space", None, None),
        P("tm", "space", None, None),
        P("space", None, None),
        P("space", None, None),
    )
    out_specs = P("tm", None, "space", None, None)
    return jax.shard_map(body, mesh=mesh, in_specs=in_specs, out_specs=out_specs, check_vma=False)
```

```python
import functools

import jax
import jax.numpy as jnp
from jax import lax
from jax.experimental import pallas as pl
from jax.experimental.pallas import tpu as pltpu
from jax.sharding import PartitionSpec as P

MESH = pl.DeviceIdType.MESH
f32 = jnp.float32

LEVELS = ((0, 4), (4, 7), (7, 13))
FORCE_LEVELS = ((0, 3), (3, 6), (6, 12))
HD = 13
SHARE = 4
ALONG_Z = 4
SC = 1.0 / 128.0
TOL = 1e-7
APPLY = 28


def loop(lo, hi, body, init, unroll):
    n = hi - lo
    if n <= unroll:
        return lax.fori_loop(lo, hi, body, init, unroll=n)
    rest = n % unroll
    init = lax.fori_loop(lo, hi - rest, body, init, unroll=unroll)
    return lax.fori_loop(hi - rest, hi, body, init, unroll=rest) if rest else init


class Solver:
    def __init__(self):
        self.inverse, self.column, self.factor = [], [], []

    def grow(self, rows):
        for row in rows:
            i = len(self.inverse)
            row = list(row)
            size = row[i]
            factors = []
            for k in range(i):
                f = row[k] * self.inverse[k]
                factors.append(f)
                for j in range(k + 1, i):
                    row[j] = row[j] - f * self.column[k][j - k - 1]
                row[i] = row[i] - f * row[k]
            for k in range(i):
                self.column[k].append(row[k])
                self.factor[k].append(factors[k])
            good = row[i] > TOL * size
            self.inverse.append(jnp.where(good, 1.0 / jnp.where(good, row[i], 1.0), 0.0))
            self.column.append([])
            self.factor.append([])

    def solve(self, g):
        g, n = list(g), len(g)
        for k in range(n):
            for i in range(k + 1, n):
                g[i] = g[i] - self.factor[k][i - k - 1] * g[k]
        y = [None] * n
        for k in reversed(range(n)):
            y[k] = g[k] * self.inverse[k]
            for i in range(k + 1, n):
                y[k] = y[k] - self.factor[k][i - k - 1] * y[i]
        return y


def kernel(ns, nt, nz, cp_hbm, co_hbm, cond_hbm, force_hbm, out_hbm, X, C, F, WZ, WY, WX, WL, E, V, W, CP, CO, CR, O,
           row_buf, gather, load_sem, out_sem, halo_send, halo_recv, chip_send, chip_recv, far_send, far_recv, share_send, share_recv, shift_send, shift_recv, ar_send, ar_recv):
    ny, nx = X.shape[1:]
    s = lax.axis_index("space")
    t = lax.axis_index("tm")
    a, b = HD, HD + nz
    has_left, has_right = s > 0, s < ns - 1

    loads = [
        pltpu.make_async_copy(co_hbm, CO, load_sem.at[0]),
        pltpu.make_async_copy(cond_hbm, C.at[pl.ds(a, nz)], load_sem.at[1]),
        pltpu.make_async_copy(force_hbm, F.at[pl.ds(a, nz)], load_sem.at[2]),
        pltpu.make_async_copy(cp_hbm, CP, load_sem.at[3]),
    ]
    for c in loads:
        c.start()

    barrier = pltpu.get_barrier_semaphore()
    for d in range(1, ns):
        pl.semaphore_signal(barrier, inc=1, device_id={"space": lax.rem(s + d, ns)}, device_id_type=MESH)

    @pl.when(t > 0)
    def _():
        pl.semaphore_signal(barrier, inc=1, device_id={"tm": lax.rem(t + nt - 1, nt)}, device_id_type=MESH)

    @pl.when(t < nt - 1)
    def _():
        pl.semaphore_signal(barrier, inc=1, device_id={"tm": lax.rem(t + 1, nt)}, device_id_type=MESH)

    quarter = t // ALONG_Z

    def sharer(d):
        first = quarter - lax.rem(quarter, SHARE)
        return (first + lax.rem(quarter + d, SHARE)) * ALONG_Z + lax.rem(t, ALONG_Z)

    for d in range(1, SHARE):
        pl.semaphore_signal(barrier, inc=1, device_id={"tm": sharer(d)}, device_id_type=MESH)

    zero = jnp.zeros((ny, nx), f32)

    def clear(lo, hi):
        def body(k, carry):
            X[k] = zero
            C[k] = zero
            F[k] = zero
            return carry

        lax.fori_loop(lo, hi, body, 0)

    @pl.when(jnp.logical_not(has_left))
    def _():
        clear(0, a)

    @pl.when(jnp.logical_not(has_right))
    def _():
        clear(b, b + HD)

    @pl.when(t == 0)
    def _():
        def body(k, carry):
            CR[k] = zero
            return carry

        lax.fori_loop(0, nz, body, 0)

    pl.semaphore_wait(barrier, (ns - 1) + (SHARE - 1) + (t > 0).astype(jnp.int32) + (t < nt - 1).astype(jnp.int32))

    edge = LEVELS[0][1]
    pieces = ((0, edge), (nz - edge, edge), (edge, nz - 2 * edge))

    def shift(i):
        p = pl.ds(*pieces[i])
        return pltpu.make_async_remote_copy(
            CO.at[p], CR.at[p], shift_send.at[i], shift_recv.at[i],
            device_id={"tm": lax.rem(t + 1, nt)}, device_id_type=MESH,
        )

    def halo(level, side):
        d0, d1 = LEVELS[level]
        if side == 0:
            src, dst, to = b - d1, a - d1, lax.rem(s + 1, ns)
        else:
            src, dst, to = a + d0, b + d0, lax.rem(s + ns - 1, ns)
        i = level * 2 + side
        return pltpu.make_async_remote_copy(
            X.at[pl.ds(src, d1 - d0)], X.at[pl.ds(dst, d1 - d0)], halo_send.at[i], halo_recv.at[i],
            device_id={"space": to}, device_id_type=MESH,
        )

    def send_halo(level):
        @pl.when(has_right)
        def _():
            halo(level, 0).start()

        @pl.when(has_left)
        def _():
            halo(level, 1).start()

    def wait_halo(level, sent):
        @pl.when(has_right if sent else has_left)
        def _():
            c = halo(level, 0)
            c.wait_send() if sent else c.wait_recv()

        @pl.when(has_left if sent else has_right)
        def _():
            c = halo(level, 1)
            c.wait_send() if sent else c.wait_recv()

    odd = lax.rem(s, 2)
    outside = jnp.logical_and(has_left, has_right)
    depths = ((LEVELS[0], (LEVELS[1][0], LEVELS[2][1])), (FORCE_LEVELS[0], (FORCE_LEVELS[1][0], FORCE_LEVELS[2][1])))
    my_rows = pl.ds(pl.multiple_of(lax.rem(quarter, SHARE) * (ny // SHARE), 8), ny // SHARE)

    def chip_copy(field, part):
        d0, d1 = depths[field][part]
        ref = (C, F)[field]
        src = odd * (a + d0) + (1 - odd) * (b - d1)
        dst = odd * (b + d0) + (1 - odd) * (a - d1)
        i = field * 2 + part
        return pltpu.make_async_remote_copy(
            ref.at[pl.ds(src, d1 - d0)], ref.at[pl.ds(dst, d1 - d0)], chip_send.at[i], chip_recv.at[i],
            device_id={"space": s + 1 - 2 * odd}, device_id_type=MESH,
        )

    def far_copy(field, part):
        d0, d1 = depths[field][part]
        ref = (C, F)[field]
        src = odd * (b - d1) + (1 - odd) * (a + d0)
        dst = odd * (a - d1) + (1 - odd) * (b + d0)
        i = field * 2 + part
        return pltpu.make_async_remote_copy(
            ref.at[pl.ds(src, d1 - d0), my_rows], ref.at[pl.ds(dst, d1 - d0), my_rows], far_send.at[i], far_recv.at[i],
            device_id={"space": lax.rem(s + ns - 1 + 2 * odd, ns)}, device_id_type=MESH,
        )

    def share_copy(field, part, d):
        d0, d1 = depths[field][part]
        ref = (C, F)[field]
        here = odd * (b + d0) + (1 - odd) * (a - d1)
        p = ref.at[pl.ds(here, d1 - d0), my_rows]
        i = (field * 2 + part) * (SHARE - 1) + d - 1
        return pltpu.make_async_remote_copy(
            p, p, share_send.at[i], share_recv.at[i], device_id={"tm": sharer(d)}, device_id_type=MESH
        )

    def send_inputs(part):
        for f in range(2):
            chip_copy(f, part).start()

        @pl.when(outside)
        def _():
            for f in range(2):
                far_copy(f, part).start()

    def pass_inputs(part):
        @pl.when(outside)
        def _():
            for f in range(2):
                far_copy(f, part).wait_recv()
                for d in range(1, SHARE):
                    share_copy(f, part, d).start()

    def wait_inputs(part):
        for f in range(2):
            chip_copy(f, part).wait_recv()

        @pl.when(outside)
        def _():
            for f in range(2):
                for d in range(1, SHARE):
                    share_copy(f, part, d).wait_recv()

    def wait_inputs_sent():
        for part in range(2):
            for f in range(2):
                chip_copy(f, part).wait_send()

        @pl.when(outside)
        def _():
            for part in range(2):
                for f in range(2):
                    far_copy(f, part).wait_send()
                    for d in range(1, SHARE):
                        share_copy(f, part, d).wait_send()

    loads[1].wait()
    loads[2].wait()
    send_inputs(0)
    loads[0].wait()

    @pl.when(t < nt - 1)
    def _():
        for i in range(3):
            shift(i).start()

    send_inputs(1)

    edge_y = lax.broadcasted_iota(jnp.int32, (ny, nx), 0)
    edge_x = lax.broadcasted_iota(jnp.int32, (ny, nx), 1)
    outer = ((edge_y == 0).astype(f32) + (edge_y == ny - 1).astype(f32)
             + (edge_x == 0).astype(f32) + (edge_x == nx - 1).astype(f32))
    keep_y = (edge_y < ny - 1).astype(f32) * (2 * SC)
    keep_x = (edge_x < nx - 1).astype(f32) * (2 * SC)
    keep_l = (edge_x > 0).astype(f32) * (2 * SC)
    outer = outer * (2 * SC)

    def plane_weights(lo, hi):
        def body(k, carry):
            c = C[k]
            WY[k] = keep_y * (c + pltpu.roll(c, ny - 1, 0))
            WX[k] = keep_x * (c + pltpu.roll(c, nx - 1, 1))
            WL[k] = keep_l * (c + pltpu.roll(c, 1, 1))
            E[k] = SC + outer * c
            return carry

        loop(lo, hi, body, 0, 6)

    def face_weights(lo, hi):
        def body(k, carry):
            WZ[k] = (2 * SC) * (C[k - 1] + C[k])
            return carry

        loop(lo, hi, body, 0, 2)

    def apply(src, dst, lo, hi, finish=None):
        def body(k, below):
            v = src(k)
            above = WZ[k + 1] * (src(k + 1) - v)
            fy = WY[k] * (pltpu.roll(v, ny - 1, 0) - v)
            fx = WX[k] * (pltpu.roll(v, nx - 1, 1) - v) + WL[k] * (pltpu.roll(v, 1, 1) - v)
            out = E[k] * v - ((above - below) + (fy - pltpu.roll(fy, 1, 0)) + fx)
            dst(k, out, v)
            return above

        loop(lo, hi, body, WZ[lo] * (src(lo) - src(lo - 1)), APPLY)

    def from_x(k):
        return X[k]

    def start_residual(k, image, v):
        V[0, k] = (v + 0.25 * F[k]) - 128.0 * image

    def power(buf, j, lo, hi):
        def put(k, image, v):
            buf[j, k] = image

        apply(lambda k: buf[j - 1, k], put, lo, hi)

    def dots(pairs, used):
        def body(k, accs):
            val = {u: (V if u[0] == "v" else W)[int(u[1]), k] for u in used}
            out = []
            for acc, (p, q) in zip(accs, pairs):
                z = val[p] * val[q]
                out.append(acc + ((z[0:8] + z[8:16]) + (z[16:24] + z[24:32])))
            return tuple(out)

        return loop(a, b, body, tuple(jnp.zeros((8, nx), f32) for _ in pairs), 2)

    lane = lax.broadcasted_iota(jnp.int32, (1, 128), 1)

    def to_row(accs):
        r = jnp.zeros((1, 128), f32)
        for n, acc in enumerate(accs):
            total = jnp.sum(jnp.sum(acc, axis=0, keepdims=True), axis=1, keepdims=True)
            r = jnp.where(lane == n, jnp.broadcast_to(total, (1, 128)), r)
        return r

    def exchange(n, d):
        return pltpu.make_async_remote_copy(
            row_buf.at[n], gather.at[n, s], ar_send.at[n], ar_recv.at[n],
            device_id={"space": lax.rem(s + d, ns)}, device_id_type=MESH,
        )

    def all_rows(n, sem):
        p = gather.at[n, pl.ds(0, ns - 1)]
        return pltpu.make_async_copy(p, p, sem.at[n])

    order = sorted(range(1, ns), key=lambda d: -min(d, ns - d))

    def send_row(n, r):
        row_buf[n] = r
        for d in order:
            exchange(n, d).start()

    def totals(n, r, pairs):
        all_rows(n, ar_recv).wait()
        parts = [jnp.where(s == q, r, gather[n, q]) for q in range(ns)]
        while len(parts) > 1:
            parts = [parts[i] + parts[i + 1] for i in range(0, len(parts), 2)]
        total = jnp.broadcast_to(parts[0], (8, 128))
        return {p: jnp.broadcast_to(total[:, i : i + 1], (8, 128)) for i, p in enumerate(pairs)}

    def own_pairs(u):
        return [(u + "0", u + "0"), (u + "0", u + "1"), (u + "0", u + "2"), (u + "1", u + "1"), (u + "1", u + "2"),
                (u + "2", u + "2"), (u + "2", u + "3")]

    def own_rows(m, u):
        return [[m[u + "0", u + "1"]], [m[u + "1", u + "1"], m[u + "1", u + "2"]],
                [m[u + "1", u + "2"], m[u + "2", u + "2"], m[u + "2", u + "3"]]]

    def own_side(m, u):
        return [m[u + "0", u + "0"], m[u + "0", u + "1"], m[u + "0", u + "2"]]

    first_pairs = own_pairs("v")
    second_pairs = [("w0", "v0")] + [(f"w{i}", f"v{j}") for i in range(3) for j in (1, 2, 3)] + own_pairs("w")

    def spread(y):
        return jnp.concatenate([y] * (ny // 8), axis=0)

    def next_residual(coefs, lo, hi):
        def body(k, carry):
            W[0, k] = V[0, k] - (coefs[0] * V[1, k] + coefs[1] * V[2, k] + coefs[2] * V[3, k])
            return carry

        loop(lo, hi, body, 0, 2)

    def both_sides(f, d0, d1):
        f(a - d1, a - d0)
        f(b + d0, b + d1)

    def more_weights(d0, d1):
        both_sides(plane_weights, d0, d1)
        face_weights(a - d1, a - d0)
        face_weights(b + d0 + 1, b + d1 + 1)

    def residual(lo, hi):
        apply(from_x, start_residual, lo, hi)

    def powers(buf, d0, d1, last):
        for j in range(1, last + 1):
            both_sides(functools.partial(power, buf, j), d0 - j, d1 - j)

    def section(which, before=None):
        residual(a - 3, b + 3)
        for j in (1, 2, 3):
            power(V, j, a - 3 + j, b + 3 - j)
        r = to_row(dots(first_pairs, ("v0", "v1", "v2", "v3")))
        send_row(2 * which, r)
        if which == 0:
            send_halo(2)
            wait_inputs(1)
            wait_halo(1, False)
            more_weights(3, 6)
        else:
            before()
        both_sides(residual, 3, 6)
        powers(V, 3, 6, 3)
        m = totals(2 * which, r, first_pairs)
        solver = Solver()
        solver.grow(own_rows(m, "v"))
        y1 = solver.solve(own_side(m, "v"))
        coefs = [spread(y) for y in y1]
        next_residual(coefs, a - 3, b + 3)
        for j in (1, 2, 3):
            power(W, j, a - 3 + j, b + 3 - j)
        r = to_row(dots(second_pairs, ("v0", "v1", "v2", "v3", "w0", "w1", "w2", "w3")))
        send_row(2 * which + 1, r)
        if which == 0:
            wait_halo(2, False)
            more_weights(6, 12)
            both_sides(residual, 6, 12)
            powers(V, 6, 12, 3)
            both_sides(functools.partial(next_residual, coefs), 3, 9)
            powers(W, 3, 9, 2)
        m = totals(2 * which + 1, r, second_pairs)
        solver.grow([[m[f"w{i}", f"v{j}"] for j in (1, 2, 3)] + row for i, row in enumerate(own_rows(m, "w"))])
        y2 = solver.solve([m["w0", "v0"], m["w0", "v1"], m["w0", "v2"]] + own_side(m, "w"))
        cv = [spread((y1[j] + y2[j]) * SC) for j in range(3)]
        cw = [spread(y2[3 + j] * SC) for j in range(3)]

        def result(k):
            v = (cv[0] * V[0, k] + cv[1] * V[1, k]) + cv[2] * V[2, k]
            w = (cw[0] * W[0, k] + cw[1] * W[1, k]) + cw[2] * W[2, k]
            return X[k] + (v + w)

        return result

    loads[3].wait()

    def add(k, carry):
        X[a + k] = CP[k] + CR[k]
        return carry

    def arrive(i):
        @pl.when(t > 0)
        def _():
            shift(i).wait_recv()

        loop(pieces[i][0], sum(pieces[i]), add, 0, 4)

    pass_inputs(0)
    arrive(0)
    arrive(1)
    send_halo(0)
    arrive(2)
    send_halo(1)
    pass_inputs(1)

    wait_inputs(0)
    plane_weights(a - 3, b + 3)
    face_weights(a - 3, b + 4)

    @pl.when(jnp.logical_not(has_left))
    def _():
        WZ[a] = zero
        E[a] = E[a] + (2 * SC) * C[a]

    @pl.when(jnp.logical_not(has_right))
    def _():
        WZ[b] = zero
        E[b - 1] = E[b - 1] + (2 * SC) * C[b - 1]

    wait_halo(0, False)

    result = section(0)
    for level in range(3):
        wait_halo(level, True)

    def put_x(k, carry):
        X[k] = result0(k)
        return carry

    result0 = result
    loop(a - 4, b + 4, put_x, 0, 4)
    out0 = pltpu.make_async_copy(X.at[pl.ds(a, nz)], out_hbm.at[0], out_sem.at[0])
    out0.start()
    result = section(1, lambda: both_sides(lambda lo, hi: loop(lo, hi, put_x, 0, 3), 4, 7))

    def put_o(k, carry):
        O[k] = result(a + k)
        return carry

    loop(0, nz, put_o, 0, 4)
    out1 = pltpu.make_async_copy(O, out_hbm.at[1], out_sem.at[1])
    out1.start()

    wait_inputs_sent()
    for n in range(4):
        all_rows(n, ar_send).wait()

    @pl.when(t < nt - 1)
    def _():
        for i in range(3):
            shift(i).wait_send()

    out0.wait()
    out1.wait()


def solution(mesh):
    ns, nt = mesh.shape["space"], mesh.shape["tm"]

    def body(c_points, corrections, conductivity, forcing):
        nz, ny, nx = conductivity.shape
        ext = nz + 2 * HD
        out = pl.pallas_call(
            functools.partial(kernel, ns, nt, nz),
            out_shape=jax.ShapeDtypeStruct((2, nz, ny, nx), f32),
            in_specs=[pl.BlockSpec(memory_space=pl.ANY)] * 4,
            out_specs=pl.BlockSpec(memory_space=pl.ANY),
            scratch_shapes=[
                pltpu.VMEM((ext, ny, nx), f32),
                pltpu.VMEM((ext, ny, nx), f32),
                pltpu.VMEM((ext, ny, nx), f32),
                pltpu.VMEM((ext + 1, ny, nx), f32),
                pltpu.VMEM((ext, ny, nx), f32),
                pltpu.VMEM((ext, ny, nx), f32),
                pltpu.VMEM((ext, ny, nx), f32),
                pltpu.VMEM((ext, ny, nx), f32),
                pltpu.VMEM((4, ext, ny, nx), f32),
                pltpu.VMEM((4, ext, ny, nx), f32),
                pltpu.VMEM((nz, ny, nx), f32),
                pltpu.VMEM((nz, ny, nx), f32),
                pltpu.VMEM((nz, ny, nx), f32),
                pltpu.VMEM((nz, ny, nx), f32),
                pltpu.VMEM((4, 1, 128), f32),
                pltpu.VMEM((4, ns, 1, 128), f32),
                pltpu.SemaphoreType.DMA((4,)),
                pltpu.SemaphoreType.DMA((2,)),
                pltpu.SemaphoreType.DMA((6,)),
                pltpu.SemaphoreType.DMA((6,)),
                pltpu.SemaphoreType.DMA((4,)),
                pltpu.SemaphoreType.DMA((4,)),
                pltpu.SemaphoreType.DMA((4,)),
                pltpu.SemaphoreType.DMA((4,)),
                pltpu.SemaphoreType.DMA((4 * (SHARE - 1),)),
                pltpu.SemaphoreType.DMA((4 * (SHARE - 1),)),
                pltpu.SemaphoreType.DMA((3,)),
                pltpu.SemaphoreType.DMA((3,)),
                pltpu.SemaphoreType.DMA((4,)),
                pltpu.SemaphoreType.DMA((4,)),
            ],
            compiler_params=pltpu.CompilerParams(collective_id=0, has_side_effects=True),
        )(c_points[0], corrections[0], conductivity, forcing)
        return out[None]

    in_specs = (
        P("tm", "space", None, None),
        P("tm", "space", None, None),
        P("space", None, None),
        P("space", None, None),
    )
    out_specs = P("tm", None, "space", None, None)
    return jax.shard_map(body, mesh=mesh, in_specs=in_specs, out_specs=out_specs, check_vma=False)
```

```python
import functools

import jax
import jax.numpy as jnp
from jax import lax
from jax.experimental import pallas as pl
from jax.experimental.pallas import tpu as pltpu
from jax.sharding import PartitionSpec as P

MESH = pl.DeviceIdType.MESH
f32 = jnp.float32

LEVELS = ((0, 4), (4, 7), (7, 13))
FORCE_LEVELS = ((0, 3), (3, 6), (6, 12))
HD = 13
SHARE = 4
ALONG_Z = 4
SC = 1.0 / 128.0
TOL = 1e-7
APPLY = 28


def loop(lo, hi, body, init, unroll):
    n = hi - lo
    if n <= unroll:
        return lax.fori_loop(lo, hi, body, init, unroll=n)
    rest = n % unroll
    init = lax.fori_loop(lo, hi - rest, body, init, unroll=unroll)
    return lax.fori_loop(hi - rest, hi, body, init, unroll=rest) if rest else init


class Solver:
    def __init__(self):
        self.inverse, self.column, self.factor = [], [], []

    def grow(self, rows):
        for row in rows:
            i = len(self.inverse)
            row = list(row)
            size = row[i]
            factors = []
            for k in range(i):
                f = row[k] * self.inverse[k]
                factors.append(f)
                for j in range(k + 1, i):
                    row[j] = row[j] - f * self.column[k][j - k - 1]
                row[i] = row[i] - f * row[k]
            for k in range(i):
                self.column[k].append(row[k])
                self.factor[k].append(factors[k])
            good = row[i] > TOL * size
            self.inverse.append(jnp.where(good, 1.0 / jnp.where(good, row[i], 1.0), 0.0))
            self.column.append([])
            self.factor.append([])

    def solve(self, g):
        g, n = list(g), len(g)
        for k in range(n):
            for i in range(k + 1, n):
                g[i] = g[i] - self.factor[k][i - k - 1] * g[k]
        y = [None] * n
        for k in reversed(range(n)):
            y[k] = g[k] * self.inverse[k]
            for i in range(k + 1, n):
                y[k] = y[k] - self.factor[k][i - k - 1] * y[i]
        return y


def kernel(ns, nt, nz, cp_hbm, co_hbm, cond_hbm, force_hbm, out_hbm, X, C, F, WZ, WY, WX, WL, E, V, W, CP, CO, CR, O,
           row_buf, gather, load_sem, out_sem, halo_send, halo_recv, chip_send, chip_recv, far_send, far_recv, share_send, share_recv, shift_send, shift_recv, ar_send, ar_recv):
    ny, nx = X.shape[1:]
    s = lax.axis_index("space")
    t = lax.axis_index("tm")
    a, b = HD, HD + nz
    has_left, has_right = s > 0, s < ns - 1

    loads = [
        pltpu.make_async_copy(co_hbm, CO, load_sem.at[0]),
        pltpu.make_async_copy(cond_hbm, C.at[pl.ds(a, nz)], load_sem.at[1]),
        pltpu.make_async_copy(force_hbm, F.at[pl.ds(a, nz)], load_sem.at[2]),
        pltpu.make_async_copy(cp_hbm, CP, load_sem.at[3]),
    ]
    for c in loads:
        c.start()

    barrier = pltpu.get_barrier_semaphore()
    for d in range(1, ns):
        pl.semaphore_signal(barrier, inc=1, device_id={"space": lax.rem(s + d, ns)}, device_id_type=MESH)

    @pl.when(t > 0)
    def _():
        pl.semaphore_signal(barrier, inc=1, device_id={"tm": lax.rem(t + nt - 1, nt)}, device_id_type=MESH)

    @pl.when(t < nt - 1)
    def _():
        pl.semaphore_signal(barrier, inc=1, device_id={"tm": lax.rem(t + 1, nt)}, device_id_type=MESH)

    quarter = t // ALONG_Z

    def sharer(d):
        first = quarter - lax.rem(quarter, SHARE)
        return (first + lax.rem(quarter + d, SHARE)) * ALONG_Z + lax.rem(t, ALONG_Z)

    for d in range(1, SHARE):
        pl.semaphore_signal(barrier, inc=1, device_id={"tm": sharer(d)}, device_id_type=MESH)

    zero = jnp.zeros((ny, nx), f32)

    def clear(lo, hi):
        def body(k, carry):
            X[k] = zero
            C[k] = zero
            F[k] = zero
            return carry

        lax.fori_loop(lo, hi, body, 0)

    @pl.when(jnp.logical_not(has_left))
    def _():
        clear(0, a)

    @pl.when(jnp.logical_not(has_right))
    def _():
        clear(b, b + HD)

    @pl.when(t == 0)
    def _():
        def body(k, carry):
            CR[k] = zero
            return carry

        lax.fori_loop(0, nz, body, 0)

    pl.semaphore_wait(barrier, (ns - 1) + (SHARE - 1) + (t > 0).astype(jnp.int32) + (t < nt - 1).astype(jnp.int32))

    edge = LEVELS[0][1]
    pieces = ((0, edge), (nz - edge, edge), (edge, nz - 2 * edge))

    def shift(i):
        p = pl.ds(*pieces[i])
        return pltpu.make_async_remote_copy(
            CO.at[p], CR.at[p], shift_send.at[i], shift_recv.at[i],
            device_id={"tm": lax.rem(t + 1, nt)}, device_id_type=MESH,
        )

    def halo(level, side):
        d0, d1 = LEVELS[level]
        if side == 0:
            src, dst, to = b - d1, a - d1, lax.rem(s + 1, ns)
        else:
            src, dst, to = a + d0, b + d0, lax.rem(s + ns - 1, ns)
        i = level * 2 + side
        return pltpu.make_async_remote_copy(
            X.at[pl.ds(src, d1 - d0)], X.at[pl.ds(dst, d1 - d0)], halo_send.at[i], halo_recv.at[i],
            device_id={"space": to}, device_id_type=MESH,
        )

    def send_halo(level):
        @pl.when(has_right)
        def _():
            halo(level, 0).start()

        @pl.when(has_left)
        def _():
            halo(level, 1).start()

    def wait_halo(level, sent):
        @pl.when(has_right if sent else has_left)
        def _():
            c = halo(level, 0)
            c.wait_send() if sent else c.wait_recv()

        @pl.when(has_left if sent else has_right)
        def _():
            c = halo(level, 1)
            c.wait_send() if sent else c.wait_recv()

    odd = lax.rem(s, 2)
    outside = jnp.logical_and(has_left, has_right)
    depths = ((LEVELS[0], (LEVELS[1][0], LEVELS[2][1])), (FORCE_LEVELS[0], (FORCE_LEVELS[1][0], FORCE_LEVELS[2][1])))
    my_rows = pl.ds(pl.multiple_of(lax.rem(quarter, SHARE) * (ny // SHARE), 8), ny // SHARE)

    def chip_copy(field, part):
        d0, d1 = depths[field][part]
        ref = (C, F)[field]
        src = odd * (a + d0) + (1 - odd) * (b - d1)
        dst = odd * (b + d0) + (1 - odd) * (a - d1)
        i = field * 2 + part
        return pltpu.make_async_remote_copy(
            ref.at[pl.ds(src, d1 - d0)], ref.at[pl.ds(dst, d1 - d0)], chip_send.at[i], chip_recv.at[i],
            device_id={"space": s + 1 - 2 * odd}, device_id_type=MESH,
        )

    def far_copy(field, part):
        d0, d1 = depths[field][part]
        ref = (C, F)[field]
        src = odd * (b - d1) + (1 - odd) * (a + d0)
        dst = odd * (a - d1) + (1 - odd) * (b + d0)
        i = field * 2 + part
        return pltpu.make_async_remote_copy(
            ref.at[pl.ds(src, d1 - d0), my_rows], ref.at[pl.ds(dst, d1 - d0), my_rows], far_send.at[i], far_recv.at[i],
            device_id={"space": lax.rem(s + ns - 1 + 2 * odd, ns)}, device_id_type=MESH,
        )

    def share_copy(field, part, d):
        d0, d1 = depths[field][part]
        ref = (C, F)[field]
        here = odd * (b + d0) + (1 - odd) * (a - d1)
        p = ref.at[pl.ds(here, d1 - d0), my_rows]
        i = (field * 2 + part) * (SHARE - 1) + d - 1
        return pltpu.make_async_remote_copy(
            p, p, share_send.at[i], share_recv.at[i], device_id={"tm": sharer(d)}, device_id_type=MESH
        )

    def send_inputs(part):
        for f in range(2):
            chip_copy(f, part).start()

        @pl.when(outside)
        def _():
            for f in range(2):
                far_copy(f, part).start()

    def pass_inputs(part):
        @pl.when(outside)
        def _():
            for f in range(2):
                far_copy(f, part).wait_recv()
                for d in range(1, SHARE):
                    share_copy(f, part, d).start()

    def wait_inputs(part):
        for f in range(2):
            chip_copy(f, part).wait_recv()

        @pl.when(outside)
        def _():
            for f in range(2):
                for d in range(1, SHARE):
                    share_copy(f, part, d).wait_recv()

    def wait_inputs_sent():
        for part in range(2):
            for f in range(2):
                chip_copy(f, part).wait_send()

        @pl.when(outside)
        def _():
            for part in range(2):
                for f in range(2):
                    far_copy(f, part).wait_send()
                    for d in range(1, SHARE):
                        share_copy(f, part, d).wait_send()

    loads[1].wait()
    loads[2].wait()
    send_inputs(0)
    loads[0].wait()

    @pl.when(t < nt - 1)
    def _():
        for i in range(3):
            shift(i).start()

    send_inputs(1)

    edge_y = lax.broadcasted_iota(jnp.int32, (ny, nx), 0)
    edge_x = lax.broadcasted_iota(jnp.int32, (ny, nx), 1)
    outer = ((edge_y == 0).astype(f32) + (edge_y == ny - 1).astype(f32)
             + (edge_x == 0).astype(f32) + (edge_x == nx - 1).astype(f32))
    keep_y = (edge_y < ny - 1).astype(f32) * (2 * SC)
    keep_x = (edge_x < nx - 1).astype(f32) * (2 * SC)
    keep_l = (edge_x > 0).astype(f32) * (2 * SC)
    outer = outer * (2 * SC)

    def plane_weights(lo, hi):
        def body(k, carry):
            c = C[k]
            WY[k] = keep_y * (c + pltpu.roll(c, ny - 1, 0))
            WX[k] = keep_x * (c + pltpu.roll(c, nx - 1, 1))
            WL[k] = keep_l * (c + pltpu.roll(c, 1, 1))
            E[k] = SC + outer * c
            return carry

        loop(lo, hi, body, 0, 6)

    def face_weights(lo, hi):
        def body(k, carry):
            WZ[k] = (2 * SC) * (C[k - 1] + C[k])
            return carry

        loop(lo, hi, body, 0, 2)

    def apply(src, dst, lo, hi, finish=None):
        def body(k, below):
            v = src(k)
            above = WZ[k + 1] * (src(k + 1) - v)
            fy = WY[k] * (pltpu.roll(v, ny - 1, 0) - v)
            fx = WX[k] * (pltpu.roll(v, nx - 1, 1) - v) + WL[k] * (pltpu.roll(v, 1, 1) - v)
            out = E[k] * v - ((above - below) + (fy - pltpu.roll(fy, 1, 0)) + fx)
            dst(k, out, v)
            return above

        loop(lo, hi, body, WZ[lo] * (src(lo) - src(lo - 1)), APPLY)

    def from_x(k):
        return X[k]

    def start_residual(k, image, v):
        V[0, k] = (v + 0.25 * F[k]) - 128.0 * image

    def power(buf, j, lo, hi):
        def put(k, image, v):
            buf[j, k] = image

        apply(lambda k: buf[j - 1, k], put, lo, hi)

    def dots(pairs, used):
        def body(k, accs):
            val = {u: (V if u[0] == "v" else W)[int(u[1]), k] for u in used}
            out = []
            for acc, (p, q) in zip(accs, pairs):
                z = val[p] * val[q]
                out.append(acc + ((z[0:8] + z[8:16]) + (z[16:24] + z[24:32])))
            return tuple(out)

        return loop(a, b, body, tuple(jnp.zeros((8, nx), f32) for _ in pairs), 16)

    lane = lax.broadcasted_iota(jnp.int32, (1, 128), 1)

    def to_row(accs):
        r = jnp.zeros((1, 128), f32)
        for n, acc in enumerate(accs):
            total = jnp.sum(jnp.sum(acc, axis=0, keepdims=True), axis=1, keepdims=True)
            r = jnp.where(lane == n, jnp.broadcast_to(total, (1, 128)), r)
        return r

    def exchange(n, d):
        return pltpu.make_async_remote_copy(
            row_buf.at[n], gather.at[n, s], ar_send.at[n], ar_recv.at[n],
            device_id={"space": lax.rem(s + d, ns)}, device_id_type=MESH,
        )

    def all_rows(n, sem):
        p = gather.at[n, pl.ds(0, ns - 1)]
        return pltpu.make_async_copy(p, p, sem.at[n])

    order = sorted(range(1, ns), key=lambda d: -min(d, ns - d))

    def send_row(n, r):
        row_buf[n] = r
        for d in order:
            exchange(n, d).start()

    def totals(n, r, pairs):
        all_rows(n, ar_recv).wait()
        parts = [jnp.where(s == q, r, gather[n, q]) for q in range(ns)]
        while len(parts) > 1:
            parts = [parts[i] + parts[i + 1] for i in range(0, len(parts), 2)]
        total = jnp.broadcast_to(parts[0], (8, 128))
        return {p: jnp.broadcast_to(total[:, i : i + 1], (8, 128)) for i, p in enumerate(pairs)}

    def own_pairs(u):
        return [(u + "0", u + "0"), (u + "0", u + "1"), (u + "0", u + "2"), (u + "1", u + "1"), (u + "1", u + "2"),
                (u + "2", u + "2"), (u + "2", u + "3")]

    def own_rows(m, u):
        return [[m[u + "0", u + "1"]], [m[u + "1", u + "1"], m[u + "1", u + "2"]],
                [m[u + "1", u + "2"], m[u + "2", u + "2"], m[u + "2", u + "3"]]]

    def own_side(m, u):
        return [m[u + "0", u + "0"], m[u + "0", u + "1"], m[u + "0", u + "2"]]

    first_pairs = own_pairs("v")
    second_pairs = [("w0", "v0")] + [(f"w{i}", f"v{j}") for i in range(3) for j in (1, 2, 3)] + own_pairs("w")

    def spread(y):
        return jnp.concatenate([y] * (ny // 8), axis=0)

    def next_residual(coefs, lo, hi):
        def body(k, carry):
            W[0, k] = V[0, k] - (coefs[0] * V[1, k] + coefs[1] * V[2, k] + coefs[2] * V[3, k])
            return carry

        loop(lo, hi, body, 0, 8)

    def both_sides(f, d0, d1):
        f(a - d1, a - d0)
        f(b + d0, b + d1)

    def more_weights(d0, d1):
        both_sides(plane_weights, d0, d1)
        face_weights(a - d1, a - d0)
        face_weights(b + d0 + 1, b + d1 + 1)

    def residual(lo, hi):
        apply(from_x, start_residual, lo, hi)

    def powers(buf, d0, d1, last):
        for j in range(1, last + 1):
            both_sides(functools.partial(power, buf, j), d0 - j, d1 - j)

    def section(which, before=None):
        residual(a - 3, b + 3)
        for j in (1, 2, 3):
            power(V, j, a - 3 + j, b + 3 - j)
        r = to_row(dots(first_pairs, ("v0", "v1", "v2", "v3")))
        send_row(2 * which, r)
        if which == 0:
            send_halo(2)
            wait_inputs(1)
            wait_halo(1, False)
            more_weights(3, 6)
        else:
            before()
        both_sides(residual, 3, 6)
        powers(V, 3, 6, 3)
        m = totals(2 * which, r, first_pairs)
        solver = Solver()
        solver.grow(own_rows(m, "v"))
        y1 = solver.solve(own_side(m, "v"))
        coefs = [spread(y) for y in y1]
        next_residual(coefs, a - 3, b + 3)
        for j in (1, 2, 3):
            power(W, j, a - 3 + j, b + 3 - j)
        r = to_row(dots(second_pairs, ("v0", "v1", "v2", "v3", "w0", "w1", "w2", "w3")))
        send_row(2 * which + 1, r)
        if which == 0:
            wait_halo(2, False)
            more_weights(6, 12)
            both_sides(residual, 6, 12)
            powers(V, 6, 12, 3)
            both_sides(functools.partial(next_residual, coefs), 3, 9)
            powers(W, 3, 9, 2)
        m = totals(2 * which + 1, r, second_pairs)
        solver.grow([[m[f"w{i}", f"v{j}"] for j in (1, 2, 3)] + row for i, row in enumerate(own_rows(m, "w"))])
        y2 = solver.solve([m["w0", "v0"], m["w0", "v1"], m["w0", "v2"]] + own_side(m, "w"))
        cv = [spread((y1[j] + y2[j]) * SC) for j in range(3)]
        cw = [spread(y2[3 + j] * SC) for j in range(3)]

        def result(k):
            v = (cv[0] * V[0, k] + cv[1] * V[1, k]) + cv[2] * V[2, k]
            w = (cw[0] * W[0, k] + cw[1] * W[1, k]) + cw[2] * W[2, k]
            return X[k] + (v + w)

        return result

    loads[3].wait()

    def add(k, carry):
        X[a + k] = CP[k] + CR[k]
        return carry

    def arrive(i):
        @pl.when(t > 0)
        def _():
            shift(i).wait_recv()

        loop(pieces[i][0], sum(pieces[i]), add, 0, 4)

    arrive(0)
    arrive(1)
    send_halo(0)
    pass_inputs(0)
    arrive(2)
    send_halo(1)
    pass_inputs(1)

    wait_inputs(0)
    plane_weights(a - 3, b + 3)
    face_weights(a - 3, b + 4)

    @pl.when(jnp.logical_not(has_left))
    def _():
        WZ[a] = zero
        E[a] = E[a] + (2 * SC) * C[a]

    @pl.when(jnp.logical_not(has_right))
    def _():
        WZ[b] = zero
        E[b - 1] = E[b - 1] + (2 * SC) * C[b - 1]

    wait_halo(0, False)

    result = section(0)
    for level in range(3):
        wait_halo(level, True)

    def put_x(k, carry):
        X[k] = result0(k)
        return carry

    result0 = result
    loop(a - 4, b + 4, put_x, 0, 4)
    out0 = pltpu.make_async_copy(X.at[pl.ds(a, nz)], out_hbm.at[0], out_sem.at[0])
    out0.start()
    result = section(1, lambda: both_sides(lambda lo, hi: loop(lo, hi, put_x, 0, 3), 4, 7))

    def put_o(k, carry):
        O[k] = result(a + k)
        return carry

    loop(0, nz, put_o, 0, 8)
    out1 = pltpu.make_async_copy(O, out_hbm.at[1], out_sem.at[1])
    out1.start()

    wait_inputs_sent()
    for n in range(4):
        all_rows(n, ar_send).wait()

    @pl.when(t < nt - 1)
    def _():
        for i in range(3):
            shift(i).wait_send()

    out0.wait()
    out1.wait()


def solution(mesh):
    ns, nt = mesh.shape["space"], mesh.shape["tm"]

    def body(c_points, corrections, conductivity, forcing):
        nz, ny, nx = conductivity.shape
        ext = nz + 2 * HD
        out = pl.pallas_call(
            functools.partial(kernel, ns, nt, nz),
            out_shape=jax.ShapeDtypeStruct((2, nz, ny, nx), f32),
            in_specs=[pl.BlockSpec(memory_space=pl.ANY)] * 4,
            out_specs=pl.BlockSpec(memory_space=pl.ANY),
            scratch_shapes=[
                pltpu.VMEM((ext, ny, nx), f32),
                pltpu.VMEM((ext, ny, nx), f32),
                pltpu.VMEM((ext, ny, nx), f32),
                pltpu.VMEM((ext + 1, ny, nx), f32),
                pltpu.VMEM((ext, ny, nx), f32),
                pltpu.VMEM((ext, ny, nx), f32),
                pltpu.VMEM((ext, ny, nx), f32),
                pltpu.VMEM((ext, ny, nx), f32),
                pltpu.VMEM((4, ext, ny, nx), f32),
                pltpu.VMEM((4, ext, ny, nx), f32),
                pltpu.VMEM((nz, ny, nx), f32),
                pltpu.VMEM((nz, ny, nx), f32),
                pltpu.VMEM((nz, ny, nx), f32),
                pltpu.VMEM((nz, ny, nx), f32),
                pltpu.VMEM((4, 1, 128), f32),
                pltpu.VMEM((4, ns, 1, 128), f32),
                pltpu.SemaphoreType.DMA((4,)),
                pltpu.SemaphoreType.DMA((2,)),
                pltpu.SemaphoreType.DMA((6,)),
                pltpu.SemaphoreType.DMA((6,)),
                pltpu.SemaphoreType.DMA((4,)),
                pltpu.SemaphoreType.DMA((4,)),
                pltpu.SemaphoreType.DMA((4,)),
                pltpu.SemaphoreType.DMA((4,)),
                pltpu.SemaphoreType.DMA((4 * (SHARE - 1),)),
                pltpu.SemaphoreType.DMA((4 * (SHARE - 1),)),
                pltpu.SemaphoreType.DMA((3,)),
                pltpu.SemaphoreType.DMA((3,)),
                pltpu.SemaphoreType.DMA((4,)),
                pltpu.SemaphoreType.DMA((4,)),
            ],
            compiler_params=pltpu.CompilerParams(collective_id=0, has_side_effects=True),
        )(c_points[0], corrections[0], conductivity, forcing)
        return out[None]

    in_specs = (
        P("tm", "space", None, None),
        P("tm", "space", None, None),
        P("space", None, None),
        P("space", None, None),
    )
    out_specs = P("tm", None, "space", None, None)
    return jax.shard_map(body, mesh=mesh, in_specs=in_specs, out_specs=out_specs, check_vma=False)
```

```python
import functools

import jax
import jax.numpy as jnp
from jax import lax
from jax.experimental import pallas as pl
from jax.experimental.pallas import tpu as pltpu
from jax.sharding import PartitionSpec as P

MESH = pl.DeviceIdType.MESH
f32 = jnp.float32

LEVELS = ((0, 4), (4, 7), (7, 13))
FORCE_LEVELS = ((0, 3), (3, 6), (6, 12))
HD = 13
SHARE = 4
ALONG_Z = 4
SC = 1.0 / 128.0
TOL = 1e-7
APPLY = 28


def loop(lo, hi, body, init, unroll):
    n = hi - lo
    if n <= unroll:
        return lax.fori_loop(lo, hi, body, init, unroll=n)
    rest = n % unroll
    init = lax.fori_loop(lo, hi - rest, body, init, unroll=unroll)
    return lax.fori_loop(hi - rest, hi, body, init, unroll=rest) if rest else init


class Solver:
    def __init__(self):
        self.inverse, self.column, self.factor = [], [], []

    def grow(self, rows):
        for row in rows:
            i = len(self.inverse)
            row = list(row)
            size = row[i]
            factors = []
            for k in range(i):
                f = row[k] * self.inverse[k]
                factors.append(f)
                for j in range(k + 1, i):
                    row[j] = row[j] - f * self.column[k][j - k - 1]
                row[i] = row[i] - f * row[k]
            for k in range(i):
                self.column[k].append(row[k])
                self.factor[k].append(factors[k])
            good = row[i] > TOL * size
            self.inverse.append(jnp.where(good, 1.0 / jnp.where(good, row[i], 1.0), 0.0))
            self.column.append([])
            self.factor.append([])

    def solve(self, g):
        g, n = list(g), len(g)
        for k in range(n):
            for i in range(k + 1, n):
                g[i] = g[i] - self.factor[k][i - k - 1] * g[k]
        y = [None] * n
        for k in reversed(range(n)):
            y[k] = g[k] * self.inverse[k]
            for i in range(k + 1, n):
                y[k] = y[k] - self.factor[k][i - k - 1] * y[i]
        return y


def kernel(ns, nt, nz, cp_hbm, co_hbm, cond_hbm, force_hbm, out_hbm, X, C, F, WZ, WY, WX, WL, E, V, W, CP, CO, CR, O,
           row_buf, gather, load_sem, out_sem, halo_send, halo_recv, chip_send, chip_recv, far_send, far_recv, share_send, share_recv, shift_send, shift_recv, ar_send, ar_recv):
    ny, nx = X.shape[1:]
    s = lax.axis_index("space")
    t = lax.axis_index("tm")
    a, b = HD, HD + nz
    has_left, has_right = s > 0, s < ns - 1

    loads = [
        pltpu.make_async_copy(co_hbm, CO, load_sem.at[0]),
        pltpu.make_async_copy(cond_hbm, C.at[pl.ds(a, nz)], load_sem.at[1]),
        pltpu.make_async_copy(force_hbm, F.at[pl.ds(a, nz)], load_sem.at[2]),
        pltpu.make_async_copy(cp_hbm, CP, load_sem.at[3]),
    ]
    for c in loads:
        c.start()

    barrier = pltpu.get_barrier_semaphore()
    for d in range(1, ns):
        pl.semaphore_signal(barrier, inc=1, device_id={"space": lax.rem(s + d, ns)}, device_id_type=MESH)

    @pl.when(t > 0)
    def _():
        pl.semaphore_signal(barrier, inc=1, device_id={"tm": lax.rem(t + nt - 1, nt)}, device_id_type=MESH)

    @pl.when(t < nt - 1)
    def _():
        pl.semaphore_signal(barrier, inc=1, device_id={"tm": lax.rem(t + 1, nt)}, device_id_type=MESH)

    quarter = t // ALONG_Z

    def sharer(d):
        first = quarter - lax.rem(quarter, SHARE)
        return (first + lax.rem(quarter + d, SHARE)) * ALONG_Z + lax.rem(t, ALONG_Z)

    for d in range(1, SHARE):
        pl.semaphore_signal(barrier, inc=1, device_id={"tm": sharer(d)}, device_id_type=MESH)

    zero = jnp.zeros((ny, nx), f32)

    def clear(lo, hi):
        def body(k, carry):
            X[k] = zero
            C[k] = zero
            F[k] = zero
            return carry

        lax.fori_loop(lo, hi, body, 0)

    @pl.when(jnp.logical_not(has_left))
    def _():
        clear(0, a)

    @pl.when(jnp.logical_not(has_right))
    def _():
        clear(b, b + HD)

    @pl.when(t == 0)
    def _():
        def body(k, carry):
            CR[k] = zero
            return carry

        lax.fori_loop(0, nz, body, 0)

    pl.semaphore_wait(barrier, (ns - 1) + (SHARE - 1) + (t > 0).astype(jnp.int32) + (t < nt - 1).astype(jnp.int32))

    edge = LEVELS[0][1]
    pieces = ((0, edge), (nz - edge, edge), (edge, nz - 2 * edge))

    def shift(i):
        p = pl.ds(*pieces[i])
        return pltpu.make_async_remote_copy(
            CO.at[p], CR.at[p], shift_send.at[i], shift_recv.at[i],
            device_id={"tm": lax.rem(t + 1, nt)}, device_id_type=MESH,
        )

    def halo(level, side):
        d0, d1 = LEVELS[level]
        if side == 0:
            src, dst, to = b - d1, a - d1, lax.rem(s + 1, ns)
        else:
            src, dst, to = a + d0, b + d0, lax.rem(s + ns - 1, ns)
        i = level * 2 + side
        return pltpu.make_async_remote_copy(
            X.at[pl.ds(src, d1 - d0)], X.at[pl.ds(dst, d1 - d0)], halo_send.at[i], halo_recv.at[i],
            device_id={"space": to}, device_id_type=MESH,
        )

    def send_halo(level):
        @pl.when(has_right)
        def _():
            halo(level, 0).start()

        @pl.when(has_left)
        def _():
            halo(level, 1).start()

    def wait_halo(level, sent):
        @pl.when(has_right if sent else has_left)
        def _():
            c = halo(level, 0)
            c.wait_send() if sent else c.wait_recv()

        @pl.when(has_left if sent else has_right)
        def _():
            c = halo(level, 1)
            c.wait_send() if sent else c.wait_recv()

    odd = lax.rem(s, 2)
    outside = jnp.logical_and(has_left, has_right)
    depths = ((LEVELS[0], (LEVELS[1][0], LEVELS[2][1])), (FORCE_LEVELS[0], (FORCE_LEVELS[1][0], FORCE_LEVELS[2][1])))
    my_rows = pl.ds(pl.multiple_of(lax.rem(quarter, SHARE) * (ny // SHARE), 8), ny // SHARE)

    def chip_copy(field, part):
        d0, d1 = depths[field][part]
        ref = (C, F)[field]
        src = odd * (a + d0) + (1 - odd) * (b - d1)
        dst = odd * (b + d0) + (1 - odd) * (a - d1)
        i = field * 2 + part
        return pltpu.make_async_remote_copy(
            ref.at[pl.ds(src, d1 - d0)], ref.at[pl.ds(dst, d1 - d0)], chip_send.at[i], chip_recv.at[i],
            device_id={"space": s + 1 - 2 * odd}, device_id_type=MESH,
        )

    def far_copy(field, part):
        d0, d1 = depths[field][part]
        ref = (C, F)[field]
        src = odd * (b - d1) + (1 - odd) * (a + d0)
        dst = odd * (a - d1) + (1 - odd) * (b + d0)
        i = field * 2 + part
        return pltpu.make_async_remote_copy(
            ref.at[pl.ds(src, d1 - d0), my_rows], ref.at[pl.ds(dst, d1 - d0), my_rows], far_send.at[i], far_recv.at[i],
            device_id={"space": lax.rem(s + ns - 1 + 2 * odd, ns)}, device_id_type=MESH,
        )

    def share_copy(field, part, d):
        d0, d1 = depths[field][part]
        ref = (C, F)[field]
        here = odd * (b + d0) + (1 - odd) * (a - d1)
        p = ref.at[pl.ds(here, d1 - d0), my_rows]
        i = (field * 2 + part) * (SHARE - 1) + d - 1
        return pltpu.make_async_remote_copy(
            p, p, share_send.at[i], share_recv.at[i], device_id={"tm": sharer(d)}, device_id_type=MESH
        )

    def send_inputs(part):
        for f in range(2):
            chip_copy(f, part).start()

        @pl.when(outside)
        def _():
            for f in range(2):
                far_copy(f, part).start()

    def pass_inputs(part):
        @pl.when(outside)
        def _():
            for f in range(2):
                far_copy(f, part).wait_recv()
                for d in range(1, SHARE):
                    share_copy(f, part, d).start()

    def wait_inputs(part):
        for f in range(2):
            chip_copy(f, part).wait_recv()

        @pl.when(outside)
        def _():
            for f in range(2):
                for d in range(1, SHARE):
                    share_copy(f, part, d).wait_recv()

    def wait_inputs_sent():
        for part in range(2):
            for f in range(2):
                chip_copy(f, part).wait_send()

        @pl.when(outside)
        def _():
            for part in range(2):
                for f in range(2):
                    far_copy(f, part).wait_send()
                    for d in range(1, SHARE):
                        share_copy(f, part, d).wait_send()

    loads[1].wait()
    loads[2].wait()
    send_inputs(0)
    loads[0].wait()

    @pl.when(t < nt - 1)
    def _():
        for i in range(3):
            shift(i).start()

    send_inputs(1)

    edge_y = lax.broadcasted_iota(jnp.int32, (ny, nx), 0)
    edge_x = lax.broadcasted_iota(jnp.int32, (ny, nx), 1)
    outer = ((edge_y == 0).astype(f32) + (edge_y == ny - 1).astype(f32)
             + (edge_x == 0).astype(f32) + (edge_x == nx - 1).astype(f32))
    keep_y = (edge_y < ny - 1).astype(f32) * (2 * SC)
    keep_x = (edge_x < nx - 1).astype(f32) * (2 * SC)
    keep_l = (edge_x > 0).astype(f32) * (2 * SC)
    outer = outer * (2 * SC)

    def plane_weights(lo, hi):
        def body(k, carry):
            c = C[k]
            WY[k] = keep_y * (c + pltpu.roll(c, ny - 1, 0))
            WX[k] = keep_x * (c + pltpu.roll(c, nx - 1, 1))
            WL[k] = keep_l * (c + pltpu.roll(c, 1, 1))
            E[k] = SC + outer * c
            return carry

        loop(lo, hi, body, 0, 6)

    def face_weights(lo, hi):
        def body(k, carry):
            WZ[k] = (2 * SC) * (C[k - 1] + C[k])
            return carry

        loop(lo, hi, body, 0, 2)

    def apply(src, dst, lo, hi, finish=None):
        def body(k, below):
            v = src(k)
            above = WZ[k + 1] * (src(k + 1) - v)
            fy = WY[k] * (pltpu.roll(v, ny - 1, 0) - v)
            fx = WX[k] * (pltpu.roll(v, nx - 1, 1) - v) + WL[k] * (pltpu.roll(v, 1, 1) - v)
            out = E[k] * v - ((above - below) + (fy - pltpu.roll(fy, 1, 0)) + fx)
            dst(k, out, v)
            return above

        loop(lo, hi, body, WZ[lo] * (src(lo) - src(lo - 1)), APPLY)

    def from_x(k):
        return X[k]

    def start_residual(k, image, v):
        V[0, k] = (v + 0.25 * F[k]) - 128.0 * image

    def power(buf, j, lo, hi):
        def put(k, image, v):
            buf[j, k] = image

        apply(lambda k: buf[j - 1, k], put, lo, hi)

    def dots(pairs, used):
        def body(k, accs):
            val = {u: (V if u[0] == "v" else W)[int(u[1]), k] for u in used}
            out = []
            for acc, (p, q) in zip(accs, pairs):
                z = val[p] * val[q]
                out.append(acc + ((z[0:8] + z[8:16]) + (z[16:24] + z[24:32])))
            return tuple(out)

        return loop(a, b, body, tuple(jnp.zeros((8, nx), f32) for _ in pairs), 16)

    lane = lax.broadcasted_iota(jnp.int32, (1, 128), 1)

    def to_row(accs):
        r = jnp.zeros((1, 128), f32)
        for n, acc in enumerate(accs):
            total = jnp.sum(jnp.sum(acc, axis=0, keepdims=True), axis=1, keepdims=True)
            r = jnp.where(lane == n, jnp.broadcast_to(total, (1, 128)), r)
        return r

    def exchange(n, d):
        return pltpu.make_async_remote_copy(
            row_buf.at[n], gather.at[n, s], ar_send.at[n], ar_recv.at[n],
            device_id={"space": lax.rem(s + d, ns)}, device_id_type=MESH,
        )

    def all_rows(n, sem):
        p = gather.at[n, pl.ds(0, ns - 1)]
        return pltpu.make_async_copy(p, p, sem.at[n])

    order = sorted(range(1, ns), key=lambda d: -min(d, ns - d))

    def send_row(n, r):
        row_buf[n] = r
        for d in order:
            exchange(n, d).start()

    def totals(n, r, pairs):
        all_rows(n, ar_recv).wait()
        parts = [jnp.where(s == q, r, gather[n, q]) for q in range(ns)]
        while len(parts) > 1:
            parts = [parts[i] + parts[i + 1] for i in range(0, len(parts), 2)]
        total = jnp.broadcast_to(parts[0], (8, 128))
        return {p: jnp.broadcast_to(total[:, i : i + 1], (8, 128)) for i, p in enumerate(pairs)}

    def own_pairs(u):
        return [(u + "0", u + "0"), (u + "0", u + "1"), (u + "0", u + "2"), (u + "1", u + "1"), (u + "1", u + "2"),
                (u + "2", u + "2"), (u + "2", u + "3")]

    def own_rows(m, u):
        return [[m[u + "0", u + "1"]], [m[u + "1", u + "1"], m[u + "1", u + "2"]],
                [m[u + "1", u + "2"], m[u + "2", u + "2"], m[u + "2", u + "3"]]]

    def own_side(m, u):
        return [m[u + "0", u + "0"], m[u + "0", u + "1"], m[u + "0", u + "2"]]

    first_pairs = own_pairs("v")
    second_pairs = [("w0", "v0")] + [(f"w{i}", f"v{j}") for i in range(3) for j in (1, 2, 3)] + own_pairs("w")

    def spread(y):
        return jnp.concatenate([y] * (ny // 8), axis=0)

    def next_residual(coefs, lo, hi):
        def body(k, carry):
            W[0, k] = V[0, k] - (coefs[0] * V[1, k] + coefs[1] * V[2, k] + coefs[2] * V[3, k])
            return carry

        loop(lo, hi, body, 0, 8)

    def both_sides(f, d0, d1):
        f(a - d1, a - d0)
        f(b + d0, b + d1)

    def more_weights(d0, d1):
        both_sides(plane_weights, d0, d1)
        face_weights(a - d1, a - d0)
        face_weights(b + d0 + 1, b + d1 + 1)

    def residual(lo, hi):
        apply(from_x, start_residual, lo, hi)

    def powers(buf, d0, d1, last):
        for j in range(1, last + 1):
            both_sides(functools.partial(power, buf, j), d0 - j, d1 - j)

    def section(which, before=None):
        if which == 0:
            residual(a - 3, a + 1)
            residual(b - 1, b + 3)
            for j in (1, 2, 3):
                power(V, j, a - 3 + j, a + 1 + j)
                power(V, j, b - 1 - j, b + 3 - j)
        else:
            residual(a - 3, b + 3)
            for j in (1, 2, 3):
                power(V, j, a - 3 + j, b + 3 - j)
        r = to_row(dots(first_pairs, ("v0", "v1", "v2", "v3")))
        send_row(2 * which, r)
        if which == 0:
            send_halo(2)
            wait_inputs(1)
            wait_halo(1, False)
            more_weights(3, 6)
        else:
            before()
        both_sides(residual, 3, 6)
        powers(V, 3, 6, 3)
        m = totals(2 * which, r, first_pairs)
        solver = Solver()
        solver.grow(own_rows(m, "v"))
        y1 = solver.solve(own_side(m, "v"))
        coefs = [spread(y) for y in y1]
        next_residual(coefs, a - 3, b + 3)
        for j in (1, 2, 3):
            power(W, j, a - 3 + j, b + 3 - j)
        r = to_row(dots(second_pairs, ("v0", "v1", "v2", "v3", "w0", "w1", "w2", "w3")))
        send_row(2 * which + 1, r)
        if which == 0:
            wait_halo(2, False)
            more_weights(6, 12)
            both_sides(residual, 6, 12)
            powers(V, 6, 12, 3)
            both_sides(functools.partial(next_residual, coefs), 3, 9)
            powers(W, 3, 9, 2)
        m = totals(2 * which + 1, r, second_pairs)
        solver.grow([[m[f"w{i}", f"v{j}"] for j in (1, 2, 3)] + row for i, row in enumerate(own_rows(m, "w"))])
        y2 = solver.solve([m["w0", "v0"], m["w0", "v1"], m["w0", "v2"]] + own_side(m, "w"))
        cv = [spread((y1[j] + y2[j]) * SC) for j in range(3)]
        cw = [spread(y2[3 + j] * SC) for j in range(3)]

        def result(k):
            v = (cv[0] * V[0, k] + cv[1] * V[1, k]) + cv[2] * V[2, k]
            w = (cw[0] * W[0, k] + cw[1] * W[1, k]) + cw[2] * W[2, k]
            return X[k] + (v + w)

        return result

    loads[3].wait()

    def add(k, carry):
        X[a + k] = CP[k] + CR[k]
        return carry

    def arrive(i):
        @pl.when(t > 0)
        def _():
            shift(i).wait_recv()

        loop(pieces[i][0], sum(pieces[i]), add, 0, 4)

    plane_weights(a, b)
    face_weights(a + 1, b)
    arrive(0)
    arrive(1)
    send_halo(0)
    pass_inputs(0)
    arrive(2)
    send_halo(1)
    residual(a + 1, b - 1)
    for j in (1, 2, 3):
        power(V, j, a + 1 + j, b - 1 - j)
    pass_inputs(1)

    wait_inputs(0)
    both_sides(plane_weights, 0, 3)
    face_weights(a - 3, a + 1)
    face_weights(b, b + 4)

    @pl.when(jnp.logical_not(has_left))
    def _():
        WZ[a] = zero
        E[a] = E[a] + (2 * SC) * C[a]

    @pl.when(jnp.logical_not(has_right))
    def _():
        WZ[b] = zero
        E[b - 1] = E[b - 1] + (2 * SC) * C[b - 1]

    wait_halo(0, False)

    result = section(0)
    for level in range(3):
        wait_halo(level, True)

    def put_x(k, carry):
        X[k] = result0(k)
        return carry

    result0 = result
    loop(a - 4, b + 4, put_x, 0, 4)
    out0 = pltpu.make_async_copy(X.at[pl.ds(a, nz)], out_hbm.at[0], out_sem.at[0])
    out0.start()
    result = section(1, lambda: both_sides(lambda lo, hi: loop(lo, hi, put_x, 0, 3), 4, 7))

    def put_o(k, carry):
        O[k] = result(a + k)
        return carry

    loop(0, nz, put_o, 0, 8)
    out1 = pltpu.make_async_copy(O, out_hbm.at[1], out_sem.at[1])
    out1.start()

    wait_inputs_sent()
    for n in range(4):
        all_rows(n, ar_send).wait()

    @pl.when(t < nt - 1)
    def _():
        for i in range(3):
            shift(i).wait_send()

    out0.wait()
    out1.wait()


def solution(mesh):
    ns, nt = mesh.shape["space"], mesh.shape["tm"]

    def body(c_points, corrections, conductivity, forcing):
        nz, ny, nx = conductivity.shape
        ext = nz + 2 * HD
        out = pl.pallas_call(
            functools.partial(kernel, ns, nt, nz),
            out_shape=jax.ShapeDtypeStruct((2, nz, ny, nx), f32),
            in_specs=[pl.BlockSpec(memory_space=pl.ANY)] * 4,
            out_specs=pl.BlockSpec(memory_space=pl.ANY),
            scratch_shapes=[
                pltpu.VMEM((ext, ny, nx), f32),
                pltpu.VMEM((ext, ny, nx), f32),
                pltpu.VMEM((ext, ny, nx), f32),
                pltpu.VMEM((ext + 1, ny, nx), f32),
                pltpu.VMEM((ext, ny, nx), f32),
                pltpu.VMEM((ext, ny, nx), f32),
                pltpu.VMEM((ext, ny, nx), f32),
                pltpu.VMEM((ext, ny, nx), f32),
                pltpu.VMEM((4, ext, ny, nx), f32),
                pltpu.VMEM((4, ext, ny, nx), f32),
                pltpu.VMEM((nz, ny, nx), f32),
                pltpu.VMEM((nz, ny, nx), f32),
                pltpu.VMEM((nz, ny, nx), f32),
                pltpu.VMEM((nz, ny, nx), f32),
                pltpu.VMEM((4, 1, 128), f32),
                pltpu.VMEM((4, ns, 1, 128), f32),
                pltpu.SemaphoreType.DMA((4,)),
                pltpu.SemaphoreType.DMA((2,)),
                pltpu.SemaphoreType.DMA((6,)),
                pltpu.SemaphoreType.DMA((6,)),
                pltpu.SemaphoreType.DMA((4,)),
                pltpu.SemaphoreType.DMA((4,)),
                pltpu.SemaphoreType.DMA((4,)),
                pltpu.SemaphoreType.DMA((4,)),
                pltpu.SemaphoreType.DMA((4 * (SHARE - 1),)),
                pltpu.SemaphoreType.DMA((4 * (SHARE - 1),)),
                pltpu.SemaphoreType.DMA((3,)),
                pltpu.SemaphoreType.DMA((3,)),
                pltpu.SemaphoreType.DMA((4,)),
                pltpu.SemaphoreType.DMA((4,)),
            ],
            compiler_params=pltpu.CompilerParams(collective_id=0, has_side_effects=True),
        )(c_points[0], corrections[0], conductivity, forcing)
        return out[None]

    in_specs = (
        P("tm", "space", None, None),
        P("tm", "space", None, None),
        P("space", None, None),
        P("space", None, None),
    )
    out_specs = P("tm", None, "space", None, None)
    return jax.shard_map(body, mesh=mesh, in_specs=in_specs, out_specs=out_specs, check_vma=False)
```
